16 devices in a mesh: col: 4 (over z, y), row: 4 (over x, core).
Axes of the slice: x: 2, y: 2, z: 2, core: 2. Of those that a mesh axis runs over, the one named last changes fastest.
Arguments:
- x_in: bfloat16 [1, 96, 768, 512], P(None, 'row', 'col')
- a_pre: bfloat16 [1, 96, 768, 512], P(None, 'row', 'col')
- g_out: bfloat16 [1, 96, 768, 512], P(None, 'row', 'col')
- w_one: bfloat16 [3, 3, 512, 512], replicated
- w_two: bfloat16 [3, 3, 512, 512], replicated
Outputs:
- output 1: bfloat16 [1, 96, 768, 512], P(None, 'row', 'col')
- output 2: float32 [3, 3, 512, 512], replicated
- output 3: float32 [3, 3, 512, 512], replicated
All inputs are finite; a program needn't handle non-finite values.
Results may differ from the reference program's by a relative error of at most 0.001.
Values are sent between devices in bfloat16 or wider.
A program may use at most 1 GiB of HBM per device.

```python
import jax
import jax.numpy as jnp
from jax import lax

IMAGES = 1
CHANNELS = 512
TILE_ROWS = 24
TILE_COLS = 192
IMG_HEIGHT = 96
IMG_WIDTH = 768

FRAME_PAD = ((0, 0), (1, 1), (1, 1), (0, 0))


def conv_same(image_in, kernel):
    return lax.conv_general_dilated(image_in, kernel, (1, 1), "SAME", dimension_numbers=("NHWC", "HWIO", "NHWC"))


def gelu_slope(pre_act):
    tanh_scale = 0.7978845608028654
    cube_coef = 0.044715
    tanh_val = jnp.tanh(tanh_scale * (pre_act + cube_coef * pre_act * pre_act * pre_act))
    return 0.5 * (1.0 + tanh_val) + 0.5 * pre_act * (1.0 - tanh_val * tanh_val) * tanh_scale * (1.0 + 3.0 * cube_coef * pre_act * pre_act)


def tap_grads(left_pad, right_img):
    row_count = right_img.shape[1]
    col_count = right_img.shape[2]
    return jnp.stack([jnp.stack([jnp.einsum("bhwi,bhwo->io", left_pad[:, tap_row:tap_row + row_count, tap_col:tap_col + col_count], right_img) for tap_col in range(3)]) for tap_row in range(3)])


def edge_weight(boost):
    row_pos = jnp.arange(IMG_HEIGHT) % TILE_ROWS
    col_pos = jnp.arange(IMG_WIDTH) % TILE_COLS
    row_edge = (row_pos == 0) | (row_pos == TILE_ROWS - 1)
    col_edge = (col_pos == 0) | (col_pos == TILE_COLS - 1)
    on_edge = (row_edge[:, None] | col_edge[None, :]).astype(jnp.float32)
    return (1.0 + boost * on_edge)[None, :, :, None]


def setup_inputs(seed: int = 0) -> dict:
    key = jax.random.key(seed)
    key_x, key_a, key_g, key_one, key_two = jax.random.split(key, 5)
    img_shape = (IMAGES, IMG_HEIGHT, IMG_WIDTH, CHANNELS)
    fan_scale = (9 * CHANNELS) ** -0.5
    x_in = jax.random.normal(key_x, img_shape, jnp.float32).astype(jnp.bfloat16)
    a_pre = jax.random.normal(key_a, img_shape, jnp.float32).astype(jnp.bfloat16)
    g_out = (jax.random.normal(key_g, img_shape, jnp.float32) * edge_weight(2.0)).astype(jnp.bfloat16)
    w_one = (jax.random.normal(key_one, (3, 3, CHANNELS, CHANNELS), jnp.float32) * fan_scale).astype(jnp.bfloat16)
    w_two = (jax.random.normal(key_two, (3, 3, CHANNELS, CHANNELS), jnp.float32) * fan_scale).astype(jnp.bfloat16)
    return {"x_in": x_in, "a_pre": a_pre, "g_out": g_out, "w_one": w_one, "w_two": w_two}


def reference(x_in, a_pre, g_out, w_one, w_two):
    w_one_f = w_one.astype(jnp.float32)
    w_two_f = w_two.astype(jnp.float32)

    def conv_first(image_in):
        return conv_same(image_in, w_one_f)

    def conv_second(image_in):
        return conv_same(image_in, w_two_f)

    def one_image(packed):
        x_img, a_img, g_img = packed
        x_val = x_img[None].astype(jnp.float32)
        a_val = a_img[None].astype(jnp.float32)
        g_val = g_img[None].astype(jnp.float32)
        z_act = jax.nn.gelu(a_val, approximate=True).astype(jnp.bfloat16).astype(jnp.float32)
        d_z = jax.vjp(conv_second, z_act)[1](g_val)[0]
        d_w2 = tap_grads(jnp.pad(z_act, FRAME_PAD), g_val)
        d_a = (d_z * gelu_slope(a_val)).astype(jnp.bfloat16).astype(jnp.float32)
        conv_grad = jax.vjp(conv_first, x_val)[1](d_a)[0]
        d_w1 = tap_grads(jnp.pad(x_val, FRAME_PAD), d_a)
        d_x = (conv_grad + g_val).astype(jnp.bfloat16)
        return d_x[0], d_w1, d_w2

    d_x, w1_parts, w2_parts = lax.map(one_image, (x_in, a_pre, g_out))
    return d_x, jnp.sum(w1_parts, axis=0), jnp.sum(w2_parts, axis=0)
```

```python
import functools

import jax
import jax.numpy as jnp
from jax import lax
from jax.experimental import pallas as pl
from jax.experimental.pallas import tpu as pltpu
from jax.sharding import PartitionSpec as P

MESH = pl.DeviceIdType.MESH
F32 = jnp.float32
BF16 = jnp.bfloat16
ROWS, COLS, CH = 24, 192, 512
PIX = ROWS * COLS
GROUP = 4
GPIX = GROUP * COLS
NGROUP = ROWS // GROUP
HALVES = (256, 128, 64, 32)
SLOTS = None


def build_slots(tap=2.7, first=11.0, shift=4.5, group=4.6, xpose=3.5, dgroup=4.2, rate=46.0, lat=2.6, margin=0.0):
    msg = {1: 0.262144e6, 2: 0.131072e6, 3: 0.065536e6}
    link_free = [0.0, 0.0, 0.0]
    arrive = {}
    done_prev = {}

    def send(now, w, t, s):
        if s == 0 or s == 7:
            arrive[(w, t, s)] = now + 2.2
            return
        level = s if s <= 3 else 7 - s
        dim = (t + level - 1) % 3
        begin = max(now, link_free[dim])
        link_free[dim] = begin + msg[level] / (rate * 1e3)
        arrive[(w, t, s)] = link_free[dim] + lat

    steps = []
    for i in range(9):
        steps.append((tap + (shift if i == 3 else 0.0), (0, i)))
    for gi in range(NGROUP):
        steps.append((group, None))
    for i in range(9):
        steps.append((tap + (shift if i == 3 else 0.0) + (xpose if i == 0 else 0.0), (1, i)))
    for gi in range(NGROUP):
        steps.append((dgroup, None))
    now = first
    slots = []
    for length, made in steps:
        if made is not None and made[0] == 1:
            while any(k[:2] == (0, made[1]) for k in arrive):
                v, (w, t, s) = min((v, k) for k, v in arrive.items())
                del arrive[(w, t, s)]
                now = max(now, v) + 0.25
                slots[-1].append((w, t, s))
                if s < 7:
                    send(now, w, t, s + 1)
        now += length
        here = []
        if made is not None:
            send(now, made[0], made[1], 0)
        while True:
            ready = sorted((k[2] > 3, v, k) for k, v in arrive.items() if v + margin <= now)
            if not ready:
                break
            w, t, s = ready[0][2]
            del arrive[(w, t, s)]
            here.append((w, t, s))
            now += 0.15
            if s < 7:
                send(now, w, t, s + 1)
        slots.append(here)
    tail = []
    while arrive:
        v, (w, t, s) = min((v, k) for k, v in arrive.items())
        del arrive[(w, t, s)]
        now = max(now, v) + 0.2
        tail.append((w, t, s))
        if s < 7:
            send(now, w, t, s + 1)
    slots.append(tail)
    return slots, now


def gelu_val(a):
    return a * (0.5 * (1.0 + jnp.tanh(0.7978845608028654 * (a + 0.044715 * (a * a * a)))))


def gelu_slope(a):
    t = jnp.tanh(0.7978845608028654 * (a + 0.044715 * a * a * a))
    return 0.5 * (1.0 + t) + 0.5 * a * (1.0 - t * t) * 0.7978845608028654 * (1.0 + 3.0 * 0.044715 * a * a)


def order_of(i):
    plane = (i // 3 + 1) % 3
    row = (i % 3 + 1) % 3
    return plane, row, (2 - row) * 3 + (2 - plane)


def kernel(slots, x_ref, a_ref, g_ref, w1_ref, w2_ref, dx_ref, dw1_ref, dw2_ref,
           part, full, r0, r1, r2, r3, lhs_t, gs, wbuf, stage, edge_out, edge_in,
           send_sem, recv_sem, hs_sem, hr_sem, load_sem, stage_sem, o_sem, out_sem):
    row = lax.axis_index("row")
    col = lax.axis_index("col")
    n_row, n_col = 4, 4
    core = row % 2
    bits = (row // 2, col % 2, col // 2)
    flip = ({"row": row + 2 - 4 * (row // 2), "col": col}, {"row": row, "col": col + 1 - 2 * (col % 2)}, {"row": row, "col": col + 2 - 4 * (col // 2)})
    mate = {"row": row + 1 - 2 * core, "col": col}
    halves = (r0, r1, r2, r3)

    def when(cond):
        return pl.when(cond)

    barrier = pltpu.get_barrier_semaphore()
    for dev in (mate,) + flip:
        pl.semaphore_signal(barrier, inc=1, device_id=dev, device_id_type=MESH)
    near = ((row > 0, {"row": row - 1, "col": col}), (row < n_row - 1, {"row": row + 1, "col": col}),
            (col > 0, {"row": row, "col": col - 1}), (col < n_col - 1, {"row": row, "col": col + 1}))
    for cond, dev in near:
        @when(cond)
        def _():
            pl.semaphore_signal(barrier, inc=1, device_id=dev, device_id_type=MESH)

    g_load = pltpu.make_async_copy(g_ref, gs.at[1, pl.ds(1, ROWS)], load_sem.at[0])
    g_load.start()
    w_load = pltpu.make_async_copy(w2_ref, wbuf, load_sem.at[1])

    def stage_copy(src, chunk, slot):
        return pltpu.make_async_copy(src.at[pl.ds(pl.multiple_of(chunk * GPIX, GPIX), GPIX)], stage.at[slot], stage_sem.at[slot])

    stage_copy(a_ref, 0, 0).start()

    @when(row == 0)
    def _():
        gs[1, 0] = jnp.zeros((COLS, CH), BF16)
        gs[3, 0] = jnp.zeros((COLS, CH), BF16)

    @when(row == n_row - 1)
    def _():
        gs[1, ROWS + 1] = jnp.zeros((COLS, CH), BF16)
        gs[3, ROWS + 1] = jnp.zeros((COLS, CH), BF16)

    @when(col == 0)
    def _():
        for u in range(2):
            edge_in[u, 0] = jnp.zeros((32, CH), F32)

    @when(col == n_col - 1)
    def _():
        for u in range(2):
            edge_in[u, 1] = jnp.zeros((32, CH), F32)

    for u in range(2):
        for v in range(2):
            edge_out[u, v, 24:32] = jnp.zeros((8, CH), F32)

    pl.semaphore_wait(barrier, 8 - row // 3 - (3 - row) // 3 - col // 3 - (3 - col) // 3)

    def row_copy(u, plane, down, src=None):
        src_row, dst_row = (ROWS, 0) if down else (1, ROWS + 1)
        dev = {"row": row + 1, "col": col} if down else {"row": row - 1, "col": col}
        n = u * 4 + (0 if down else 1)
        source = gs.at[plane, src_row] if src is None else src.at[src_row - 1]
        return pltpu.make_async_remote_copy(source, gs.at[plane, dst_row], hs_sem.at[n], hr_sem.at[n], device_id=dev, device_id_type=MESH)

    def col_copy(u, right):
        dev = {"row": row, "col": col + 1} if right else {"row": row, "col": col - 1}
        n = u * 4 + (2 if right else 3)
        a, b = (1, 0) if right else (0, 1)
        return pltpu.make_async_remote_copy(edge_out.at[u, a], edge_in.at[u, b], hs_sem.at[n], hr_sem.at[n], device_id=dev, device_id_type=MESH)

    def send_rows(u, plane, src=None):
        @when(row < n_row - 1)
        def _():
            row_copy(u, plane, True, src).start()

        @when(row > 0)
        def _():
            row_copy(u, plane, False, src).start()

    def wait_rows(u, plane, src=None):
        @when(row > 0)
        def _():
            row_copy(u, plane, True, src).wait_recv()
            row_copy(u, plane, False, src).wait_send()

        @when(row < n_row - 1)
        def _():
            row_copy(u, plane, False, src).wait_recv()
            row_copy(u, plane, True, src).wait_send()

    def send_cols(u, plane):
        def body(r, _):
            edge_out[u, 0, pl.ds(r, 1)] = gs[plane, r, 0:16].astype(F32)[0:1]
            edge_out[u, 1, pl.ds(r, 1)] = gs[plane, r, COLS - 16:COLS].astype(F32)[15:16]
            return 0

        lax.fori_loop(0, ROWS + 2, body, 0)

        @when(col < n_col - 1)
        def _():
            col_copy(u, True).start()

        @when(col > 0)
        def _():
            col_copy(u, False).start()

    def wait_cols(u):
        @when(col > 0)
        def _():
            col_copy(u, True).wait_recv()
            col_copy(u, False).wait_send()

        @when(col < n_col - 1)
        def _():
            col_copy(u, False).wait_recv()
            col_copy(u, True).wait_send()

    def build_shifts(u, plane):
        spot = lax.broadcasted_iota(jnp.int32, (COLS, CH), 0)

        def body(r, _):
            val = gs[plane, r].astype(F32)
            left = edge_in[u, 0, pl.ds(r, 1)]
            right = edge_in[u, 1, pl.ds(r, 1)]
            gs[0, r] = jnp.where(spot == 0, left, pltpu.roll(val, 1, 0)).astype(BF16)
            gs[2, r] = jnp.where(spot == COLS - 1, right, pltpu.roll(val, COLS - 1, 0)).astype(BF16)
            return 0

        lax.fori_loop(0, ROWS + 2, body, 0)

    def transpose_in(src, act):
        def body(chunk, _):
            slot = chunk % 2

            @when(chunk + 1 < NGROUP)
            def _():
                stage_copy(src, chunk + 1, 1 - slot).start()

            stage_copy(src, chunk, slot).wait()
            for j in range(GPIX // 256):
                val = stage[slot, j * 256:(j + 1) * 256]
                if act:
                    val = gelu_val(val.astype(F32)).astype(BF16)
                lhs_t[:, pl.ds(pl.multiple_of(chunk * GPIX + j * 256, 256), 256)] = val.T
            return 0

        lax.fori_loop(0, NGROUP, body, 0)

    def base_of(t, level):
        off = core * 256
        for n in range(level):
            off = off + bits[(t + n) % 3] * HALVES[n + 1]
        return off

    def axis_of(t, level):
        return mate if level == 0 else flip[(t + level - 1) % 3]

    def reduce_copy(t, level, core_off=None):
        size = HALVES[level]
        if level == 0:
            off = (1 - core) * 256
        else:
            off = base_of(t, level - 1) + (1 - bits[(t + level - 1) % 3]) * size
        off = pl.multiple_of(off, 32)
        return pltpu.make_async_remote_copy(part.at[t, pl.ds(off, size)], halves[level].at[t], send_sem.at[t, level], recv_sem.at[t, level], device_id=axis_of(t, level), device_id_type=MESH)

    def gather_copy(t, level):
        size = HALVES[level]
        off = pl.multiple_of(base_of(t, level), 32)
        n = 7 - level
        return pltpu.make_async_remote_copy(full.at[t, pl.ds(off, size)], full.at[t, pl.ds(off, size)], send_sem.at[t, n], recv_sem.at[t, n], device_id=axis_of(t, level), device_id_type=MESH)

    def result_copy(w, t):
        tap = order_of(t)[2]
        return pltpu.make_async_copy(full.at[t], (dw2_ref, dw1_ref)[w].at[tap], out_sem.at[t])

    def event(w, t, s):
        if s <= 3:
            reduce_copy(t, s).wait_recv()
            size = HALVES[s]
            rows = pl.ds(pl.multiple_of(base_of(t, s), 32), size)
            (part if s < 3 else full)[t, rows] = part[t, rows] + halves[s][t]
            (reduce_copy(t, s + 1) if s < 3 else gather_copy(t, 3)).start()
        else:
            gather_copy(t, 7 - s).wait_recv()
            if s < 7:
                gather_copy(t, 6 - s).start()
            else:
                for level in range(4):
                    reduce_copy(t, level).wait_send()
                    gather_copy(t, level).wait_send()
                result_copy(w, t).start()

    def pump(i, base, count):
        for n in range(count):
            if slots[base + n]:
                @when(i == n)
                def _():
                    for w, t, s in slots[base + n]:
                        event(w, t, s)

    def tap_sum(i, plane):
        row_at = (i % 3 + 1) % 3
        grad = gs[plane, pl.ds(row_at, ROWS)].reshape(PIX, CH)
        part[i] = jnp.dot(lhs_t[...], grad, preferred_element_type=F32)
        pltpu.make_async_remote_copy(part.at[i, pl.ds(pl.multiple_of((1 - core) * 256, 256), 256)], r0.at[i], send_sem.at[i, 0], recv_sem.at[i, 0], device_id=mate, device_id_type=MESH).start()

    def conv_rows(g, center):
        top = g * GROUP
        lhs = []
        rhs = []
        for k in range(9):
            a, c = k // 3, k % 3
            plane = (0, center, 2)[2 - c]
            lhs.append(gs[plane, pl.ds(top + 2 - a, GROUP)].reshape(GPIX, CH))
            rhs.append(wbuf[k])
        return lax.dot_general(jnp.concatenate(lhs, axis=1), jnp.concatenate(rhs, axis=1), (((1,), (1,)), ((), ())), preferred_element_type=F32)

    send_rows(0, 1, g_ref)
    w_load.start()
    transpose_in(a_ref, True)
    g_load.wait()
    wait_rows(0, 1, g_ref)
    send_cols(0, 1)

    def w2_step(i, _):
        @when(i == 3)
        def _():
            wait_cols(0)
            build_shifts(0, 1)

        tap_sum(i, (i // 3 + 1) % 3)
        pump(i, 0, 9)
        return 0

    lax.fori_loop(0, 9, w2_step, 0)

    w_load.wait()

    def group_of(gi):
        return jnp.where(gi == 0, 0, jnp.where(gi == 1, NGROUP - 1, gi - 1))

    stage_copy(a_ref, 0, 0).start()

    def dz_step(gi, _):
        g = group_of(gi)
        slot = gi % 2

        @when(gi + 1 < NGROUP)
        def _():
            stage_copy(a_ref, group_of(gi + 1), 1 - slot).start()

        d_z = conv_rows(g, 1)
        stage_copy(a_ref, g, slot).wait()
        d_a = (d_z * gelu_slope(stage[slot].astype(F32))).astype(BF16)
        gs[3, pl.ds(g * GROUP + 1, GROUP)] = d_a.reshape(GROUP, COLS, CH)

        @when(gi == 1)
        def _():
            send_rows(1, 3)

        pump(gi, 9, NGROUP)
        return 0

    lax.fori_loop(0, NGROUP, dz_step, 0)
    w1_load = pltpu.make_async_copy(w1_ref, wbuf, load_sem.at[1])
    w1_load.start()
    stage_copy(x_ref, 0, 0).start()
    wait_rows(1, 3)
    send_cols(1, 3)
    transpose_in(x_ref, False)

    def w1_step(i, _):
        @when(i == 3)
        def _():
            wait_cols(1)
            build_shifts(1, 3)

        pltpu.make_async_copy(full.at[i], dw2_ref.at[0], out_sem.at[i]).wait()
        u = (i // 3 + 1) % 3
        tap_sum(i, u + 2 * u * (2 - u))
        pump(i, 15, 9)
        return 0

    lax.fori_loop(0, 9, w1_step, 0)

    w1_load.wait()

    def out_copy(g):
        return pltpu.make_async_copy(gs.at[1, pl.ds(g * GROUP + 1, GROUP)], dx_ref.at[pl.ds(g * GROUP, GROUP)], o_sem.at[g])

    def dx_step(g, _):
        rows = pl.ds(g * GROUP + 1, GROUP)
        val = conv_rows(g, 3) + gs[1, rows].reshape(GPIX, CH).astype(F32)
        gs[1, rows] = val.astype(BF16).reshape(GROUP, COLS, CH)
        out_copy(g).start()
        pump(g, 24, NGROUP)
        return 0

    lax.fori_loop(0, NGROUP, dx_step, 0)
    for w, t, s in slots[30]:
        event(w, t, s)
    for t in range(9):
        result_copy(1, t).wait()
    for g in range(NGROUP):
        out_copy(g).wait()


def solution(mesh):
    slots, _ = build_slots()

    def local_step(x_tile, a_tile, g_tile, w_one, w_two):
        any_spec = pl.BlockSpec(memory_space=pl.ANY)
        d_x, d_w1, d_w2 = pl.pallas_call(
            functools.partial(kernel, slots),
            out_shape=(jax.ShapeDtypeStruct((ROWS, COLS, CH), BF16), jax.ShapeDtypeStruct((9, CH, CH), F32), jax.ShapeDtypeStruct((9, CH, CH), F32)),
            in_specs=[any_spec] * 5,
            out_specs=[any_spec] * 3,
            scratch_shapes=[
                pltpu.VMEM((9, CH, CH), F32),
                pltpu.VMEM((9, CH, CH), F32),
                pltpu.VMEM((9, 256, CH), F32),
                pltpu.VMEM((9, 128, CH), F32),
                pltpu.VMEM((9, 64, CH), F32),
                pltpu.VMEM((9, 32, CH), F32),
                pltpu.VMEM((CH, PIX), BF16),
                pltpu.VMEM((4, ROWS + 2, COLS, CH), BF16),
                pltpu.VMEM((9, CH, CH), BF16),
                pltpu.VMEM((2, GPIX, CH), BF16),
                pltpu.VMEM((2, 2, 32, CH), F32),
                pltpu.VMEM((2, 2, 32, CH), F32),
                pltpu.SemaphoreType.DMA((9, 8)),
                pltpu.SemaphoreType.DMA((9, 8)),
                pltpu.SemaphoreType.DMA((8,)),
                pltpu.SemaphoreType.DMA((8,)),
                pltpu.SemaphoreType.DMA((2,)),
                pltpu.SemaphoreType.DMA((2,)),
                pltpu.SemaphoreType.DMA((NGROUP,)),
                pltpu.SemaphoreType.DMA((9,)),
            ],
            compiler_params=pltpu.CompilerParams(collective_id=0, has_side_effects=True, vmem_limit_bytes=67043328),
        )(x_tile.reshape(PIX, CH), a_tile.reshape(PIX, CH), g_tile.reshape(ROWS, COLS, CH), w_one.reshape(9, CH, CH), w_two.reshape(9, CH, CH))
        return d_x.reshape(1, ROWS, COLS, CH), d_w1.reshape(3, 3, CH, CH), d_w2.reshape(3, 3, CH, CH)

    tile_spec = P(None, "row", "col", None)
    return jax.shard_map(local_step, mesh=mesh, in_specs=(tile_spec, tile_spec, tile_spec, P(), P()), out_specs=(tile_spec, P(), P()), check_vma=False)
```

```python
import functools

import jax
import jax.numpy as jnp
from jax import lax
from jax.experimental import pallas as pl
from jax.experimental.pallas import tpu as pltpu
from jax.sharding import PartitionSpec as P

MESH = pl.DeviceIdType.MESH
F32 = jnp.float32
BF16 = jnp.bfloat16
ROWS, COLS, CH = 24, 192, 512
PIX = ROWS * COLS
GROUP = 2
GPIX = GROUP * COLS
NGROUP = ROWS // GROUP
HALVES = (256, 128, 64, 32)
PARTS = 2
WIDTH = CH // PARTS
SIDE = 256
ORDER = (4, 1, 7, 3, 0, 6, 5, 2, 8)


def build_slots(half=1.33, shift=2.4, dz=2.1, dx=2.0, halo=0.5, mid=0.6, first=12.7, rate=46.6, lat=2.3, hop=1.8):
    size = {1: 0.262144e3, 2: 0.131072e3, 3: 0.065536e3}
    add = (0.075, 0.04, 0.02, 0.01)
    link = [0.0, 0.0, 0.0]
    arrive = {}

    def send(now, w, t, j, s):
        if s in (0, 7):
            arrive[(w, t, j, s)] = now + hop * (0.6 + 0.4 / PARTS)
            return
        level = s if s <= 3 else 7 - s
        axis = (t + j + level - 1) % 3
        link[axis] = max(now, link[axis]) + size[level] / PARTS / rate
        arrive[(w, t, j, s)] = link[axis] + lat

    def handle(now, key):
        del arrive[key]
        w, t, j, s = key
        now += 0.03 + (add[s] / PARTS if s < 4 else 0.0)
        if s < 7:
            send(now, w, t, j, s + 1)
        return now

    steps = []
    for w in range(2):
        for n in range(18):
            steps.append((half + (shift if n == 6 else 0.0) + (halo if w and n == 0 else 0.0), (w, n)))
        steps += [((dx if w else dz), None)] * NGROUP
    now = first
    slots = []
    for index, (length, made) in enumerate(steps):
        if index == 18 + NGROUP:
            now += mid
        if made is not None and made[0] == 1 and made[1] % 2 == 0:
            while any(k[0] == 0 and k[1] == made[1] // 2 for k in arrive):
                when, key = min((v, k) for k, v in arrive.items())
                now = handle(max(now, when), key)
                slots[-1].append(key)
        now += length
        if made is not None and made[1] % 2 == 0:
            for j in range(PARTS):
                send(now + 0.1, made[0], made[1] // 2, j, 0)
        here = []
        while True:
            ready = [(k[3], v, k) for k, v in arrive.items() if v <= now and not (k[3] == 0 and made is not None and made[1] % 2 == 0 and made[1] // 2 == k[1])]
            if not ready:
                break
            key = min(ready)[2]
            now = handle(now, key)
            here.append(key)
        slots.append(here)
    tail = []
    while arrive:
        now = max(now, min(arrive.values()))
        key = min((k[3], v, k) for k, v in arrive.items() if v <= now)[2]
        now = handle(now, key)
        tail.append(key)
    slots.append(tail)
    return slots, now


def gelu_val(a):
    return a * (0.5 * (1.0 + jnp.tanh(0.7978845608028654 * (a + 0.044715 * (a * a * a)))))


def gelu_slope(a):
    t = jnp.tanh(0.7978845608028654 * (a + 0.044715 * a * a * a))
    return 0.5 * (1.0 + t) + 0.5 * a * (1.0 - t * t) * 0.7978845608028654 * (1.0 + 3.0 * 0.044715 * a * a)


def kernel(slots, x_ref, a_ref, g_ref, w1_ref, w2_ref, lv, full, dw2_ref,
           part, r0, r1, r2, r3, mid, dc, sh, wbuf, stage, dzs, edge_out, edge_in,
           send_sem, recv_sem, hs_sem, hr_sem, load_sem, stage_sem, out_sem):
    row = lax.axis_index("row")
    col = lax.axis_index("col")
    n_row, n_col = 4, 4
    core = row % 2
    bits = (row // 2, col % 2, col // 2)
    flip = ({"row": row + 2 - 4 * (row // 2), "col": col}, {"row": row, "col": col + 1 - 2 * (col % 2)}, {"row": row, "col": col + 2 - 4 * (col // 2)})
    mate = {"row": row + 1 - 2 * core, "col": col}
    halves = (r0, r1, r2, r3)

    barrier = pltpu.get_barrier_semaphore()
    for dev in (mate,) + flip:
        pl.semaphore_signal(barrier, inc=1, device_id=dev, device_id_type=MESH)
    near = ((row > 0, {"row": row - 1, "col": col}), (row < n_row - 1, {"row": row + 1, "col": col}),
            (col > 0, {"row": row, "col": col - 1}), (col < n_col - 1, {"row": row, "col": col + 1}))
    for cond, dev in near:
        @pl.when(cond)
        def _():
            pl.semaphore_signal(barrier, inc=1, device_id=dev, device_id_type=MESH)

    chunk = ROWS // 3
    a_loads = [pltpu.make_async_copy(a_ref.at[pl.ds(n * chunk, chunk)], sh.at[0, pl.ds(n * chunk, chunk)], load_sem.at[2 + n]) for n in range(3)]
    g_load = pltpu.make_async_copy(g_ref, mid.at[pl.ds(1, ROWS)], load_sem.at[0])
    w_load = pltpu.make_async_copy(w2_ref, wbuf, load_sem.at[1])
    for copy in a_loads + [g_load, w_load]:
        copy.start()

    @pl.when(row == 0)
    def _():
        mid[0] = jnp.zeros((COLS, CH), BF16)
        dc[0] = jnp.zeros((COLS, CH), BF16)

    @pl.when(row == n_row - 1)
    def _():
        mid[ROWS + 1] = jnp.zeros((COLS, CH), BF16)
        dc[ROWS + 1] = jnp.zeros((COLS, CH), BF16)

    @pl.when(col == 0)
    def _():
        for u in range(2):
            edge_in[u, 0] = jnp.zeros((32, CH), F32)

    @pl.when(col == n_col - 1)
    def _():
        for u in range(2):
            edge_in[u, 1] = jnp.zeros((32, CH), F32)

    for u in range(2):
        for v in range(2):
            edge_out[u, v, 24:32] = jnp.zeros((8, CH), F32)

    centers = (mid, dc)

    def row_copy(u, down):
        src_row, dst_row = (ROWS, 0) if down else (1, ROWS + 1)
        dev = {"row": row + 1, "col": col} if down else {"row": row - 1, "col": col}
        n = u * 4 + (0 if down else 1)
        source = dc.at[src_row] if u else g_ref.at[src_row - 1]
        return pltpu.make_async_remote_copy(source, centers[u].at[dst_row], hs_sem.at[n], hr_sem.at[n], device_id=dev, device_id_type=MESH)

    def col_copy(u, right):
        dev = {"row": row, "col": col + 1} if right else {"row": row, "col": col - 1}
        n = u * 4 + (2 if right else 3)
        a, b = (1, 0) if right else (0, 1)
        return pltpu.make_async_remote_copy(edge_out.at[u, a], edge_in.at[u, b], hs_sem.at[n], hr_sem.at[n], device_id=dev, device_id_type=MESH)

    def send_rows(u):
        @pl.when(row < n_row - 1)
        def _():
            row_copy(u, True).start()

        @pl.when(row > 0)
        def _():
            row_copy(u, False).start()

    def wait_rows(u):
        @pl.when(row > 0)
        def _():
            row_copy(u, True).wait_recv()
            row_copy(u, False).wait_send()

        @pl.when(row < n_row - 1)
        def _():
            row_copy(u, False).wait_recv()
            row_copy(u, True).wait_send()

    def send_cols(u):
        def body(r, _):
            edge_out[u, 0, pl.ds(r, 1)] = centers[u][r, 0:16].astype(F32)[0:1]
            edge_out[u, 1, pl.ds(r, 1)] = centers[u][r, COLS - 16:COLS].astype(F32)[15:16]
            return 0

        lax.fori_loop(0, ROWS + 2, body, 0)

        @pl.when(col < n_col - 1)
        def _():
            col_copy(u, True).start()

        @pl.when(col > 0)
        def _():
            col_copy(u, False).start()

    def wait_cols(u):
        @pl.when(col > 0)
        def _():
            col_copy(u, True).wait_recv()
            col_copy(u, False).wait_send()

        @pl.when(col < n_col - 1)
        def _():
            col_copy(u, False).wait_recv()
            col_copy(u, True).wait_send()

    def build_shifts(u):
        spot = lax.broadcasted_iota(jnp.int32, (COLS, CH), 0)

        def body(r, _):
            val = centers[u][r].astype(F32)
            left = edge_in[u, 0, pl.ds(r, 1)]
            right = edge_in[u, 1, pl.ds(r, 1)]
            sh[0, r] = jnp.where(spot == 0, left, pltpu.roll(val, 1, 0)).astype(BF16)
            sh[1, r] = jnp.where(spot == COLS - 1, right, pltpu.roll(val, COLS - 1, 0)).astype(BF16)
            return 0

        lax.fori_loop(0, ROWS + 2, body, 0)

    def base_of(rot, level):
        off = core * 256
        for n in range(level):
            off = off + bits[(rot + n) % 3] * HALVES[n + 1]
        return off

    def axis_of(rot, level):
        return mate if level == 0 else flip[(rot + level - 1) % 3]

    def reduce_copy(t, j, level, tap=None):
        rot = t + j
        tap = ORDER[t] if tap is None else tap
        size = HALVES[level]
        if level == 0:
            off = (1 - core) * 256
        else:
            off = base_of(rot, level - 1) + (1 - bits[(rot + level - 1) % 3]) * size
        rows, cols = pl.ds(pl.multiple_of(off, 32), size), pl.ds(j * WIDTH, WIDTH)
        return pltpu.make_async_remote_copy(part.at[tap, rows, cols], halves[level].at[tap, :, cols], send_sem.at[tap, j, level], recv_sem.at[tap, j, level], device_id=axis_of(rot, level), device_id_type=MESH)

    def gather_copy(t, j, level):
        rot, tap = t + j, ORDER[t]
        view = full.at[tap, pl.ds(pl.multiple_of(base_of(rot, level), 32), HALVES[level]), pl.ds(j * WIDTH, WIDTH)]
        n = 7 - level
        return pltpu.make_async_remote_copy(view, view, send_sem.at[tap, j, n], recv_sem.at[tap, j, n], device_id=axis_of(rot, level), device_id_type=MESH)

    def result_copy(tap, j):
        cols = pl.ds(j * WIDTH, WIDTH)
        return pltpu.make_async_copy(full.at[tap, :, cols], dw2_ref.at[tap, :, cols], out_sem.at[tap, j])

    def event(w, t, j, s):
        if s <= 3:
            reduce_copy(t, j, s).wait_recv()
            tap, cols = ORDER[t], slice(j * WIDTH, (j + 1) * WIDTH)
            rows = pl.ds(pl.multiple_of(base_of(t + j, s), 32), HALVES[s])
            (part if s < 3 else full)[tap, rows, cols] = part[tap, rows, cols] + halves[s][tap, :, cols]
            (reduce_copy(t, j, s + 1) if s < 3 else gather_copy(t, j, 3)).start()
        else:
            gather_copy(t, j, 7 - s).wait_recv()
            if s < 7:
                gather_copy(t, j, 6 - s).start()
            else:
                for level in range(4):
                    reduce_copy(t, j, level).wait_send()
                    gather_copy(t, j, level).wait_send()
                if w == 0:
                    result_copy(ORDER[t], j).start()

    def pump(n, base, lo, hi):
        if not any(slots[base + m] for m in range(lo, hi)):
            return
        if hi - lo == 1:
            for key in slots[base + lo]:
                event(*key)
            return
        half = (lo + hi) // 2

        @pl.when(n < half)
        def _():
            pump(n, base, lo, half)

        @pl.when(n >= half)
        def _():
            pump(n, base, half, hi)

    def tap_half(n, tap, row_at, plane):
        second = n % 2
        rows = pl.ds(pl.multiple_of(core * 256 + (1 - second) * (1 - 2 * core) * 256, 256), 256)
        grad = plane[pl.ds(row_at, ROWS)].reshape(PIX, CH)
        part[tap, rows] = lax.dot_general(lv[:, rows], grad, (((0,), (0,)), ((), ())), preferred_element_type=F32)

        @pl.when(second == 0)
        def _():
            for j in range(PARTS):
                reduce_copy(0, j, 0, tap).start()

    def free_tap(n, tap, again):
        if again:
            @pl.when(n % 2 == 0)
            def _():
                for j in range(PARTS):
                    result_copy(tap, j).wait()

    def tap_loops(u, base):
        def middle(n, _):
            @pl.when(n == 2)
            def _():
                if u == 0:
                    wait_rows(0)
                    send_cols(0)

            row_at = (n // 2 + 1) % 3
            tap = (2 - row_at) * 3 + 1
            free_tap(n, tap, u)
            tap_half(n, tap, row_at, centers[u])
            pump(n, base, 0, 6)
            return 0

        def side(n, _):
            which = n // 6
            row_at = (n // 2 % 3 + 1) % 3
            tap = (2 - row_at) * 3 + 2 * which
            free_tap(n, tap, u)
            tap_half(n, tap, row_at, sh.at[1 - which])
            pump(n, base + 6, 0, 12)
            return 0

        lax.fori_loop(0, 6, middle, 0)
        wait_cols(u)
        build_shifts(u)
        lax.fori_loop(0, 12, side, 0)

    def conv_rows(g, center):
        lhs = []
        rhs = []
        for k in range(9):
            a, c = k // 3, k % 3
            plane = (sh.at[1], center, sh.at[0])[c]
            lhs.append(plane[pl.ds(g * GROUP + 2 - a, GROUP)].reshape(GPIX, CH))
            rhs.append(wbuf[k])
        return lax.dot_general(jnp.concatenate(lhs, axis=1), jnp.concatenate(rhs, axis=1), (((1,), (1,)), ((), ())), preferred_element_type=F32)

    for n in range(3):
        a_loads[n].wait()

        def gelu_row(r, _):
            lv[pl.ds(pl.multiple_of(r * COLS, COLS), COLS)] = gelu_val(sh[0, r].astype(F32)).astype(BF16)
            return 0

        lax.fori_loop(n * chunk, (n + 1) * chunk, gelu_row, 0)
        if n == 0:
            pl.semaphore_wait(barrier, 8 - row // 3 - (3 - row) // 3 - col // 3 - (3 - col) // 3)
            send_rows(0)
    g_load.wait()

    tap_loops(0, 0)

    x_load = pltpu.make_async_copy(x_ref, lv, load_sem.at[0])
    x_load.start()
    w_load.wait()

    def group_of(gi):
        return jnp.where(gi == 0, 0, jnp.where(gi == 1, NGROUP - 1, gi - 1))

    def stage_copy(gi, slot):
        return pltpu.make_async_copy(a_ref.at[pl.ds(group_of(gi) * GROUP, GROUP)], stage.at[slot], stage_sem.at[slot])

    def slope_rows(gi, slot):
        a_val = stage[slot].reshape(GPIX, CH).astype(F32)
        d_a = (dzs[...] * gelu_slope(a_val)).astype(BF16)
        dc[pl.ds(group_of(gi) * GROUP + 1, GROUP)] = d_a.reshape(GROUP, COLS, CH)

    stage_copy(0, 0).start()
    dzs[...] = jnp.zeros((GPIX, CH), F32)
    stage_copy(0, 0).wait()

    def dz_step(gi, _):
        before = jnp.maximum(gi - 1, 0)
        slot = before % 2

        @pl.when(gi >= 2)
        def _():
            stage_copy(before, slot).wait()

        @pl.when(gi >= 1)
        def _():
            stage_copy(gi, gi % 2).start()

        slope_rows(before, slot)
        dzs[...] = conv_rows(group_of(gi), mid)

        @pl.when(gi == 2)
        def _():
            send_rows(1)

        pump(gi, 18, 0, NGROUP)
        return 0

    lax.fori_loop(0, NGROUP, dz_step, 0)
    w1_load = pltpu.make_async_copy(w1_ref, wbuf, load_sem.at[1])
    w1_load.start()
    stage_copy(NGROUP - 1, (NGROUP - 1) % 2).wait()
    slope_rows(NGROUP - 1, (NGROUP - 1) % 2)
    wait_rows(1)
    send_cols(1)
    x_load.wait()

    tap_loops(1, 18 + NGROUP)

    w1_load.wait()

    def dx_step(g, _):
        val = conv_rows(g, dc) + mid[pl.ds(g * GROUP + 1, GROUP)].reshape(GPIX, CH).astype(F32)
        lv[pl.ds(pl.multiple_of(g * GPIX, GPIX), GPIX)] = val.astype(BF16)
        pump(g, 36 + NGROUP, 0, NGROUP)
        return 0

    lax.fori_loop(0, NGROUP, dx_step, 0)
    for key in slots[36 + 2 * NGROUP]:
        event(*key)


def write_out(lv, full, dw2_in, dx_ref, dw1_ref, dw2_ref, bounce, in_sem, out_sem):
    reads = [pltpu.make_async_copy(dw2_in.at[k], bounce.at[k], in_sem.at[k]) for k in range(9)]
    writes = [pltpu.make_async_copy(bounce.at[k], dw2_ref.at[k], out_sem.at[k]) for k in range(9)]
    writes += [pltpu.make_async_copy(full.at[k], dw1_ref.at[k], out_sem.at[9 + k]) for k in range(9)]
    writes.append(pltpu.make_async_copy(lv, dx_ref, out_sem.at[18]))
    for copy in reads + writes[9:]:
        copy.start()
    for k in range(9):
        reads[k].wait()
        writes[k].start()
    for copy in writes:
        copy.wait()


def solution(mesh):
    slots, _ = build_slots()
    any_spec = pl.BlockSpec(memory_space=pl.ANY)
    vmem_spec = pl.BlockSpec(memory_space=pltpu.VMEM)

    def local_step(x_tile, a_tile, g_tile, w_one, w_two):
        lv, full, d_w2 = pl.pallas_call(
            functools.partial(kernel, slots),
            out_shape=(pltpu.VMEM((PIX, CH), BF16), pltpu.VMEM((9, CH, CH), F32), jax.ShapeDtypeStruct((9, CH, CH), F32)),
            in_specs=[any_spec] * 5,
            out_specs=(vmem_spec, vmem_spec, any_spec),
            scratch_shapes=[
                pltpu.VMEM((9, CH, CH), F32),
                pltpu.VMEM((9, 256, CH), F32),
                pltpu.VMEM((9, 128, CH), F32),
                pltpu.VMEM((9, 64, CH), F32),
                pltpu.VMEM((9, 32, CH), F32),
                pltpu.VMEM((ROWS + 2, COLS, CH), BF16),
                pltpu.VMEM((ROWS + 2, COLS, CH), BF16),
                pltpu.VMEM((2, ROWS + 2, COLS, CH), BF16),
                pltpu.VMEM((9, CH, CH), BF16),
                pltpu.VMEM((2, GROUP, COLS, CH), BF16),
                pltpu.VMEM((GPIX, CH), F32),
                pltpu.VMEM((2, 2, 32, CH), F32),
                pltpu.VMEM((2, 2, 32, CH), F32),
                pltpu.SemaphoreType.DMA((9, PARTS, 8)),
                pltpu.SemaphoreType.DMA((9, PARTS, 8)),
                pltpu.SemaphoreType.DMA((8,)),
                pltpu.SemaphoreType.DMA((8,)),
                pltpu.SemaphoreType.DMA((5,)),
                pltpu.SemaphoreType.DMA((2,)),
                pltpu.SemaphoreType.DMA((9, PARTS)),
            ],
            compiler_params=pltpu.CompilerParams(collective_id=0, has_side_effects=True, vmem_limit_bytes=52500000),
        )(x_tile.reshape(PIX, CH), a_tile.reshape(ROWS, COLS, CH), g_tile.reshape(ROWS, COLS, CH), w_one.reshape(9, CH, CH), w_two.reshape(9, CH, CH))
        d_x, d_w1, d_w2 = pl.pallas_call(
            write_out,
            out_shape=(jax.ShapeDtypeStruct((PIX, CH), BF16), jax.ShapeDtypeStruct((9, CH, CH), F32), jax.ShapeDtypeStruct((9, CH, CH), F32)),
            in_specs=[vmem_spec, vmem_spec, any_spec],
            out_specs=[any_spec] * 3,
            scratch_shapes=[pltpu.VMEM((9, CH, CH), F32), pltpu.SemaphoreType.DMA((9,)), pltpu.SemaphoreType.DMA((19,))],
            compiler_params=pltpu.CompilerParams(vmem_limit_bytes=50000000),
        )(lv, full, d_w2)
        return d_x.reshape(1, ROWS, COLS, CH), d_w1.reshape(3, 3, CH, CH), d_w2.reshape(3, 3, CH, CH)

    tile_spec = P(None, "row", "col", None)
    return jax.shard_map(local_step, mesh=mesh, in_specs=(tile_spec, tile_spec, tile_spec, P(), P()), out_specs=(tile_spec, P(), P()), check_vma=False)
```

```python
import functools

import jax
import jax.numpy as jnp
from jax import lax
from jax.experimental import pallas as pl
from jax.experimental.pallas import tpu as pltpu
from jax.sharding import PartitionSpec as P

MESH = pl.DeviceIdType.MESH
F32 = jnp.float32
BF16 = jnp.bfloat16
mark = jax.named_scope
ROWS, COLS, CH = 24, 192, 512
PIX = ROWS * COLS
GROUP = 2
GPIX = GROUP * COLS
NGROUP = ROWS // GROUP
HALVES = (256, 128, 64, 32)
PARTS = 2
WIDTH = CH // PARTS
SIDE = 256
ORDER = (4, 1, 7, 3, 0, 6, 5, 2, 8)


def build_slots(half=1.33, shift=2.4, dz=2.1, dx=2.0, halo=0.5, mid=0.6, first=12.7, rate=46.6, lat=2.3, hop=1.8):
    size = {1: 0.262144e3, 2: 0.131072e3, 3: 0.065536e3}
    add = (0.075, 0.04, 0.02, 0.01)
    link = [0.0, 0.0, 0.0]
    arrive = {}

    def send(now, w, t, j, s):
        if s in (0, 7):
            arrive[(w, t, j, s)] = now + hop * (0.6 + 0.4 / PARTS)
            return
        level = s if s <= 3 else 7 - s
        axis = (t + j + level - 1) % 3
        link[axis] = max(now, link[axis]) + size[level] / PARTS / rate
        arrive[(w, t, j, s)] = link[axis] + lat

    def handle(now, key):
        del arrive[key]
        w, t, j, s = key
        now += 0.03 + (add[s] / PARTS if s < 4 else 0.0)
        if s < 7:
            send(now, w, t, j, s + 1)
        return now

    steps = []
    for w in range(2):
        for n in range(18):
            steps.append((half + (shift if n == 6 else 0.0) + (halo if w and n == 0 else 0.0), (w, n)))
        steps += [((dx if w else dz), None)] * NGROUP
    now = first
    slots = []
    for index, (length, made) in enumerate(steps):
        if index == 18 + NGROUP:
            now += mid
        if made is not None and made[0] == 1 and made[1] % 2 == 0:
            while any(k[0] == 0 and k[1] == made[1] // 2 for k in arrive):
                when, key = min((v, k) for k, v in arrive.items())
                now = handle(max(now, when), key)
                slots[-1].append(key)
        now += length
        if made is not None and made[1] % 2 == 0:
            for j in range(PARTS):
                send(now + 0.1, made[0], made[1] // 2, j, 0)
        here = []
        while True:
            ready = [(k[3], v, k) for k, v in arrive.items() if v <= now and not (k[3] == 0 and made is not None and made[1] % 2 == 0 and made[1] // 2 == k[1])]
            if not ready:
                break
            key = min(ready)[2]
            now = handle(now, key)
            here.append(key)
        slots.append(here)
    tail = []
    while arrive:
        now = max(now, min(arrive.values()))
        key = min((k[3], v, k) for k, v in arrive.items() if v <= now)[2]
        now = handle(now, key)
        tail.append(key)
    slots.append(tail)
    return slots, now


def gelu_val(a):
    return a * (0.5 * (1.0 + jnp.tanh(0.7978845608028654 * (a + 0.044715 * (a * a * a)))))


def gelu_slope(a):
    t = jnp.tanh(0.7978845608028654 * (a + 0.044715 * a * a * a))
    return 0.5 * (1.0 + t) + 0.5 * a * (1.0 - t * t) * 0.7978845608028654 * (1.0 + 3.0 * 0.044715 * a * a)


def kernel(slots, x_ref, a_ref, g_ref, w1_ref, w2_ref, lv, full, dw2_ref,
           part, r0, r1, r2, r3, mid, dc, sh, wbuf, stage, dzs, edge_out, edge_in,
           send_sem, recv_sem, hs_sem, hr_sem, load_sem, stage_sem, out_sem):
    row = lax.axis_index("row")
    col = lax.axis_index("col")
    n_row, n_col = 4, 4
    core = row % 2
    bits = (row // 2, col % 2, col // 2)
    flip = ({"row": row + 2 - 4 * (row // 2), "col": col}, {"row": row, "col": col + 1 - 2 * (col % 2)}, {"row": row, "col": col + 2 - 4 * (col // 2)})
    mate = {"row": row + 1 - 2 * core, "col": col}
    halves = (r0, r1, r2, r3)

    barrier = pltpu.get_barrier_semaphore()
    for dev in (mate,) + flip:
        pl.semaphore_signal(barrier, inc=1, device_id=dev, device_id_type=MESH)
    near = ((row > 0, {"row": row - 1, "col": col}), (row < n_row - 1, {"row": row + 1, "col": col}),
            (col > 0, {"row": row, "col": col - 1}), (col < n_col - 1, {"row": row, "col": col + 1}))
    for cond, dev in near:
        @pl.when(cond)
        def _():
            pl.semaphore_signal(barrier, inc=1, device_id=dev, device_id_type=MESH)

    chunk = ROWS // 3
    a_loads = [pltpu.make_async_copy(a_ref.at[pl.ds(n * chunk, chunk)], sh.at[0, pl.ds(n * chunk, chunk)], load_sem.at[2 + n]) for n in range(3)]
    g_load = pltpu.make_async_copy(g_ref, mid.at[pl.ds(1, ROWS)], load_sem.at[0])
    w_load = pltpu.make_async_copy(w2_ref, wbuf, load_sem.at[1])
    for copy in a_loads + [g_load, w_load]:
        copy.start()

    @pl.when(row == 0)
    def _():
        mid[0] = jnp.zeros((COLS, CH), BF16)
        dc[0] = jnp.zeros((COLS, CH), BF16)

    @pl.when(row == n_row - 1)
    def _():
        mid[ROWS + 1] = jnp.zeros((COLS, CH), BF16)
        dc[ROWS + 1] = jnp.zeros((COLS, CH), BF16)

    @pl.when(col == 0)
    def _():
        for u in range(2):
            edge_in[u, 0] = jnp.zeros((32, CH), F32)

    @pl.when(col == n_col - 1)
    def _():
        for u in range(2):
            edge_in[u, 1] = jnp.zeros((32, CH), F32)

    for u in range(2):
        for v in range(2):
            edge_out[u, v, 24:32] = jnp.zeros((8, CH), F32)

    centers = (mid, dc)

    def row_copy(u, down):
        src_row, dst_row = (ROWS, 0) if down else (1, ROWS + 1)
        dev = {"row": row + 1, "col": col} if down else {"row": row - 1, "col": col}
        n = u * 4 + (0 if down else 1)
        source = dc.at[src_row] if u else g_ref.at[src_row - 1]
        return pltpu.make_async_remote_copy(source, centers[u].at[dst_row], hs_sem.at[n], hr_sem.at[n], device_id=dev, device_id_type=MESH)

    def col_copy(u, right):
        dev = {"row": row, "col": col + 1} if right else {"row": row, "col": col - 1}
        n = u * 4 + (2 if right else 3)
        a, b = (1, 0) if right else (0, 1)
        return pltpu.make_async_remote_copy(edge_out.at[u, a], edge_in.at[u, b], hs_sem.at[n], hr_sem.at[n], device_id=dev, device_id_type=MESH)

    def send_rows(u):
        @pl.when(row < n_row - 1)
        def _():
            row_copy(u, True).start()

        @pl.when(row > 0)
        def _():
            row_copy(u, False).start()

    def wait_rows(u):
        @pl.when(row > 0)
        def _():
            row_copy(u, True).wait_recv()
            row_copy(u, False).wait_send()

        @pl.when(row < n_row - 1)
        def _():
            row_copy(u, False).wait_recv()
            row_copy(u, True).wait_send()

    def send_cols(u):
        def body(r, _):
            edge_out[u, 0, pl.ds(r, 1)] = centers[u][r, 0:16].astype(F32)[0:1]
            edge_out[u, 1, pl.ds(r, 1)] = centers[u][r, COLS - 16:COLS].astype(F32)[15:16]
            return 0

        lax.fori_loop(0, ROWS + 2, body, 0)

        @pl.when(col < n_col - 1)
        def _():
            col_copy(u, True).start()

        @pl.when(col > 0)
        def _():
            col_copy(u, False).start()

    def wait_cols(u):
        @pl.when(col > 0)
        def _():
            col_copy(u, True).wait_recv()
            col_copy(u, False).wait_send()

        @pl.when(col < n_col - 1)
        def _():
            col_copy(u, False).wait_recv()
            col_copy(u, True).wait_send()

    def build_shifts(u):
        spot = lax.broadcasted_iota(jnp.int32, (COLS, CH), 0)

        def body(r, _):
            val = centers[u][r].astype(F32)
            left = edge_in[u, 0, pl.ds(r, 1)]
            right = edge_in[u, 1, pl.ds(r, 1)]
            sh[0, r] = jnp.where(spot == 0, left, pltpu.roll(val, 1, 0)).astype(BF16)
            sh[1, r] = jnp.where(spot == COLS - 1, right, pltpu.roll(val, COLS - 1, 0)).astype(BF16)
            return 0

        lax.fori_loop(0, ROWS + 2, body, 0)

    def base_of(rot, level):
        off = core * 256
        for n in range(level):
            off = off + bits[(rot + n) % 3] * HALVES[n + 1]
        return off

    def axis_of(rot, level):
        return mate if level == 0 else flip[(rot + level - 1) % 3]

    def reduce_copy(t, j, level, tap=None):
        rot = t + j
        tap = ORDER[t] if tap is None else tap
        size = HALVES[level]
        if level == 0:
            off = (1 - core) * 256
        else:
            off = base_of(rot, level - 1) + (1 - bits[(rot + level - 1) % 3]) * size
        rows, cols = pl.ds(pl.multiple_of(off, 32), size), pl.ds(j * WIDTH, WIDTH)
        return pltpu.make_async_remote_copy(part.at[tap, rows, cols], halves[level].at[tap, :, cols], send_sem.at[tap, j, level], recv_sem.at[tap, j, level], device_id=axis_of(rot, level), device_id_type=MESH)

    def gather_copy(t, j, level):
        rot, tap = t + j, ORDER[t]
        view = full.at[tap, pl.ds(pl.multiple_of(base_of(rot, level), 32), HALVES[level]), pl.ds(j * WIDTH, WIDTH)]
        n = 7 - level
        return pltpu.make_async_remote_copy(view, view, send_sem.at[tap, j, n], recv_sem.at[tap, j, n], device_id=axis_of(rot, level), device_id_type=MESH)

    def result_copy(tap, j):
        cols = pl.ds(j * WIDTH, WIDTH)
        return pltpu.make_async_copy(full.at[tap, :, cols], dw2_ref.at[tap, :, cols], out_sem.at[tap, j])

    def event(w, t, j, s):
        if s <= 3:
            reduce_copy(t, j, s).wait_recv()
            tap, cols = ORDER[t], slice(j * WIDTH, (j + 1) * WIDTH)
            rows = pl.ds(pl.multiple_of(base_of(t + j, s), 32), HALVES[s])
            (part if s < 3 else full)[tap, rows, cols] = part[tap, rows, cols] + halves[s][tap, :, cols]
            (reduce_copy(t, j, s + 1) if s < 3 else gather_copy(t, j, 3)).start()
        else:
            gather_copy(t, j, 7 - s).wait_recv()
            if s < 7:
                gather_copy(t, j, 6 - s).start()
            else:
                for level in range(4):
                    reduce_copy(t, j, level).wait_send()
                    gather_copy(t, j, level).wait_send()
                if w == 0:
                    result_copy(ORDER[t], j).start()

    def pump(n, base, lo, hi):
        if not any(slots[base + m] for m in range(lo, hi)):
            return
        if hi - lo == 1:
            for key in slots[base + lo]:
                event(*key)
            return
        half = (lo + hi) // 2

        @pl.when(n < half)
        def _():
            pump(n, base, lo, half)

        @pl.when(n >= half)
        def _():
            pump(n, base, half, hi)

    def tap_half(n, tap, row_at, plane):
        second = n % 2
        rows = pl.ds(pl.multiple_of(core * 256 + (1 - second) * (1 - 2 * core) * 256, 256), 256)
        grad = plane[pl.ds(row_at, ROWS)].reshape(PIX, CH)
        part[tap, rows] = lax.dot_general(lv[:, rows], grad, (((0,), (0,)), ((), ())), preferred_element_type=F32)

        @pl.when(second == 0)
        def _():
            for j in range(PARTS):
                reduce_copy(0, j, 0, tap).start()

    def free_tap(n, tap, again):
        if again:
            @pl.when(n % 2 == 0)
            def _():
                for j in range(PARTS):
                    result_copy(tap, j).wait()

    def tap_loops(u, base):
        def middle(n, _):
            @pl.when(n == 2)
            def _():
                if u == 0:
                    with mark("rows"):
                        wait_rows(0)
                        send_cols(0)

            row_at = (n // 2 + 1) % 3
            tap = (2 - row_at) * 3 + 1
            with mark("free"):
                free_tap(n, tap, u)
            with mark("center"):
                tap_half(n, tap, row_at, centers[u])
            with mark("pump"):
                pump(n, base, 0, 6)
            return 0

        def side(n, _):
            which = n // 6
            row_at = (n // 2 % 3 + 1) % 3
            tap = (2 - row_at) * 3 + 2 * which
            with mark("free"):
                free_tap(n, tap, u)
            with mark("side"):
                tap_half(n, tap, row_at, sh.at[1 - which])
            with mark("pump"):
                pump(n, base + 6, 0, 12)
            return 0

        lax.fori_loop(0, 6, middle, 0)
        with mark("cols"):
            wait_cols(u)
        with mark("shifts"):
            build_shifts(u)
        lax.fori_loop(0, 12, side, 0)

    def conv_rows(g, center):
        lhs = []
        rhs = []
        for k in range(9):
            a, c = k // 3, k % 3
            plane = (sh.at[1], center, sh.at[0])[c]
            lhs.append(plane[pl.ds(g * GROUP + 2 - a, GROUP)].reshape(GPIX, CH))
            rhs.append(wbuf[k])
        return lax.dot_general(jnp.concatenate(lhs, axis=1), jnp.concatenate(rhs, axis=1), (((1,), (1,)), ((), ())), preferred_element_type=F32)

    for n in range(3):
        with mark("aload"):
            a_loads[n].wait()

        def gelu_row(r, _):
            lv[pl.ds(pl.multiple_of(r * COLS, COLS), COLS)] = gelu_val(sh[0, r].astype(F32)).astype(BF16)
            return 0

        with mark("gelu"):
            lax.fori_loop(n * chunk, (n + 1) * chunk, gelu_row, 0)
        if n == 0:
          with mark("barrier"):
            pl.semaphore_wait(barrier, 8 - row // 3 - (3 - row) // 3 - col // 3 - (3 - col) // 3)
            send_rows(0)
    g_load.wait()

    tap_loops(0, 0)

    x_load = pltpu.make_async_copy(x_ref, lv, load_sem.at[0])
    x_load.start()
    w_load.wait()

    def group_of(gi):
        return jnp.where(gi == 0, 0, jnp.where(gi == 1, NGROUP - 1, gi - 1))

    def stage_copy(gi, slot):
        return pltpu.make_async_copy(a_ref.at[pl.ds(group_of(gi) * GROUP, GROUP)], stage.at[slot], stage_sem.at[slot])

    def slope_rows(gi, slot):
        a_val = stage[slot].reshape(GPIX, CH).astype(F32)
        d_a = (dzs[...] * gelu_slope(a_val)).astype(BF16)
        dc[pl.ds(group_of(gi) * GROUP + 1, GROUP)] = d_a.reshape(GROUP, COLS, CH)

    stage_copy(0, 0).start()
    dzs[...] = jnp.zeros((GPIX, CH), F32)
    stage_copy(0, 0).wait()

    def dz_step(gi, _):
        before = jnp.maximum(gi - 1, 0)
        slot = before % 2

        @pl.when(gi >= 2)
        def _():
            stage_copy(before, slot).wait()

        @pl.when(gi >= 1)
        def _():
            stage_copy(gi, gi % 2).start()

        with mark("dz"):
            slope_rows(before, slot)
            dzs[...] = conv_rows(group_of(gi), mid)

        @pl.when(gi == 2)
        def _():
            send_rows(1)

        with mark("pump"):
            pump(gi, 18, 0, NGROUP)
        return 0

    lax.fori_loop(0, NGROUP, dz_step, 0)
    w1_load = pltpu.make_async_copy(w1_ref, wbuf, load_sem.at[1])
    w1_load.start()
    with mark("between"):
        stage_copy(NGROUP - 1, (NGROUP - 1) % 2).wait()
        slope_rows(NGROUP - 1, (NGROUP - 1) % 2)
        wait_rows(1)
        send_cols(1)
        x_load.wait()

    tap_loops(1, 18 + NGROUP)

    w1_load.wait()

    def dx_step(g, _):
        with mark("dx"):
            val = conv_rows(g, dc) + mid[pl.ds(g * GROUP + 1, GROUP)].reshape(GPIX, CH).astype(F32)
            lv[pl.ds(pl.multiple_of(g * GPIX, GPIX), GPIX)] = val.astype(BF16)
        with mark("pump"):
            pump(g, 36 + NGROUP, 0, NGROUP)
        return 0

    lax.fori_loop(0, NGROUP, dx_step, 0)
    for key in slots[36 + 2 * NGROUP]:
        with mark("e%d%d%d%d" % key):
            event(*key)


def write_out(lv, full, dw2_in, dx_ref, dw1_ref, dw2_ref, bounce, in_sem, out_sem):
    reads = [pltpu.make_async_copy(dw2_in.at[k], bounce.at[k], in_sem.at[k]) for k in range(9)]
    writes = [pltpu.make_async_copy(bounce.at[k], dw2_ref.at[k], out_sem.at[k]) for k in range(9)]
    writes += [pltpu.make_async_copy(full.at[k], dw1_ref.at[k], out_sem.at[9 + k]) for k in range(9)]
    writes.append(pltpu.make_async_copy(lv, dx_ref, out_sem.at[18]))
    for copy in reads + writes[9:]:
        copy.start()
    with mark("reads"):
        for k in range(9):
            reads[k].wait()
            writes[k].start()
    with mark("writes"):
        for copy in writes:
            copy.wait()


def solution(mesh):
    slots, _ = build_slots()
    any_spec = pl.BlockSpec(memory_space=pl.ANY)
    vmem_spec = pl.BlockSpec(memory_space=pltpu.VMEM)

    def local_step(x_tile, a_tile, g_tile, w_one, w_two):
        lv, full, d_w2 = pl.pallas_call(
            functools.partial(kernel, slots),
            out_shape=(pltpu.VMEM((PIX, CH), BF16), pltpu.VMEM((9, CH, CH), F32), pltpu.HBM((9, CH, CH), F32)),
            in_specs=[any_spec] * 5,
            out_specs=(vmem_spec, vmem_spec, any_spec),
            scratch_shapes=[
                pltpu.VMEM((9, CH, CH), F32),
                pltpu.VMEM((9, 256, CH), F32),
                pltpu.VMEM((9, 128, CH), F32),
                pltpu.VMEM((9, 64, CH), F32),
                pltpu.VMEM((9, 32, CH), F32),
                pltpu.VMEM((ROWS + 2, COLS, CH), BF16),
                pltpu.VMEM((ROWS + 2, COLS, CH), BF16),
                pltpu.VMEM((2, ROWS + 2, COLS, CH), BF16),
                pltpu.VMEM((9, CH, CH), BF16),
                pltpu.VMEM((2, GROUP, COLS, CH), BF16),
                pltpu.VMEM((GPIX, CH), F32),
                pltpu.VMEM((2, 2, 32, CH), F32),
                pltpu.VMEM((2, 2, 32, CH), F32),
                pltpu.SemaphoreType.DMA((9, PARTS, 8)),
                pltpu.SemaphoreType.DMA((9, PARTS, 8)),
                pltpu.SemaphoreType.DMA((8,)),
                pltpu.SemaphoreType.DMA((8,)),
                pltpu.SemaphoreType.DMA((5,)),
                pltpu.SemaphoreType.DMA((2,)),
                pltpu.SemaphoreType.DMA((9, PARTS)),
            ],
            compiler_params=pltpu.CompilerParams(collective_id=0, has_side_effects=True, vmem_limit_bytes=52500000),
        )(x_tile.reshape(PIX, CH), a_tile.reshape(ROWS, COLS, CH), g_tile.reshape(ROWS, COLS, CH), w_one.reshape(9, CH, CH), w_two.reshape(9, CH, CH))
        d_x, d_w1, d_w2 = pl.pallas_call(
            write_out,
            out_shape=(jax.ShapeDtypeStruct((PIX, CH), BF16), jax.ShapeDtypeStruct((9, CH, CH), F32), jax.ShapeDtypeStruct((9, CH, CH), F32)),
            in_specs=[vmem_spec, vmem_spec, any_spec],
            out_specs=[any_spec] * 3,
            scratch_shapes=[pltpu.VMEM((9, CH, CH), F32), pltpu.SemaphoreType.DMA((9,)), pltpu.SemaphoreType.DMA((19,))],
            compiler_params=pltpu.CompilerParams(vmem_limit_bytes=20000000),
        )(lv, full, d_w2)
        return d_x.reshape(1, ROWS, COLS, CH), d_w1.reshape(3, 3, CH, CH), d_w2.reshape(3, 3, CH, CH)

    tile_spec = P(None, "row", "col", None)
    return jax.shard_map(local_step, mesh=mesh, in_specs=(tile_spec, tile_spec, tile_spec, P(), P()), out_specs=(tile_spec, P(), P()), check_vma=False)
```

```python
import functools

import jax
import jax.numpy as jnp
from jax import lax
from jax.experimental import pallas as pl
from jax.experimental.pallas import tpu as pltpu
from jax.sharding import PartitionSpec as P

MESH = pl.DeviceIdType.MESH
F32 = jnp.float32
BF16 = jnp.bfloat16
mark = jax.named_scope
ROWS, COLS, CH = 24, 192, 512
PIX = ROWS * COLS
GROUP = 2
GPIX = GROUP * COLS
NGROUP = ROWS // GROUP
HALVES = (256, 128, 64, 32)
PARTS = 2
WIDTH = CH // PARTS
SIDE = 256
ORDER = (4, 1, 7, 3, 0, 6, 5, 2, 8)


def step_lengths():
    steps = []
    for w in range(2):
        extra = {0: 2.2, 1: 1.5, 2: 0.3, 6: 2.1, 12: 1.2} if w == 0 else {0: 0.85, 6: 1.2, 12: 1.2}
        steps += [(1.46 + extra.get(n, 0.0), (w, n)) for n in range(18)]
        steps += [((2.05 if w else 2.32), None)] * NGROUP
    return steps


def build_slots(rank=(0, 1, 2, 3, 4, 5, 6, 7), tail_rank=(0, 1, 2, 3, 4, 5, 6, 7), first=8.2, rate=46.6, lat=2.3, hop=1.8):
    size = {1: 0.262144e3, 2: 0.131072e3, 3: 0.065536e3}
    add = (0.075, 0.04, 0.02, 0.01)
    link = [0.0, 0.0, 0.0]
    arrive = {}

    def send(now, w, t, j, s):
        if s in (0, 7):
            arrive[(w, t, j, s)] = now + hop * (0.6 + 0.4 / PARTS)
            return
        level = s if s <= 3 else 7 - s
        axis = (t + j + level - 1) % 3
        link[axis] = max(now, link[axis]) + size[level] / PARTS / rate
        arrive[(w, t, j, s)] = link[axis] + lat

    def handle(now, key):
        del arrive[key]
        w, t, j, s = key
        now += 0.03 + (add[s] / PARTS if s < 4 else 0.0)
        if s < 7:
            send(now, w, t, j, s + 1)
        return now

    now = first
    slots = []
    for length, made in step_lengths():
        if made is not None and made[0] == 1 and made[1] % 2 == 0:
            while any(k[0] == 0 and k[1] == made[1] // 2 for k in arrive):
                when, key = min((v, k) for k, v in arrive.items())
                now = handle(max(now, when), key)
                slots[-1].append(key)
        now += length
        fresh = None
        if made is not None and made[1] % 2 == 0:
            fresh = (made[0], made[1] // 2)
            for j in range(PARTS):
                send(now + 0.1, made[0], made[1] // 2, j, 0)
        here = []
        while True:
            ready = [(rank[k[3]], v, k) for k, v in arrive.items() if v <= now and not (k[3] == 0 and k[:2] == fresh)]
            if not ready:
                break
            key = min(ready)[2]
            now = handle(now, key)
            here.append(key)
        slots.append(here)
    tail = []
    while arrive:
        now = max(now, min(arrive.values()))
        key = min((tail_rank[k[3]], v, k) for k, v in arrive.items() if v <= now)[2]
        now = handle(now, key)
        tail.append(key)
    slots.append(tail)
    return slots, now


def gate(a):
    w = (0.044715 * 0.7978845608028654) * (a * a)
    return 0.5 * jnp.tanh(a * (0.7978845608028654 + w)) + 0.5, w


def gelu_val(a):
    return a * gate(a)[0]


def gelu_slope(a):
    p, w = gate(a)
    return p + (a * p) * ((1.0 - p) * (2.0 * 0.7978845608028654 + 6.0 * w))


def kernel(slots, x_ref, a_ref, g_ref, w1_ref, w2_ref, lv, full_one, full_two,
           part, r0, r1, r2, r3, mid, dc, sh, wbuf, stage, edge_out, edge_in,
           send_sem, recv_sem, hs_sem, hr_sem, load_sem, stage_sem):
    row = lax.axis_index("row")
    col = lax.axis_index("col")
    n_row, n_col = 4, 4
    core = row % 2
    bits = (row // 2, col % 2, col // 2)
    flip = ({"row": row + 2 - 4 * (row // 2), "col": col}, {"row": row, "col": col + 1 - 2 * (col % 2)}, {"row": row, "col": col + 2 - 4 * (col // 2)})
    mate = {"row": row + 1 - 2 * core, "col": col}
    halves = (r0, r1, r2, r3)
    full = (full_two, full_one)
    dzs = full_one.at[8, pl.ds(0, GPIX)]

    barrier = pltpu.get_barrier_semaphore()
    for dev in (mate,) + flip:
        pl.semaphore_signal(barrier, inc=1, device_id=dev, device_id_type=MESH)
    near = ((row > 0, {"row": row - 1, "col": col}), (row < n_row - 1, {"row": row + 1, "col": col}),
            (col > 0, {"row": row, "col": col - 1}), (col < n_col - 1, {"row": row, "col": col + 1}))
    for cond, dev in near:
        @pl.when(cond)
        def _():
            pl.semaphore_signal(barrier, inc=1, device_id=dev, device_id_type=MESH)

    g_load = pltpu.make_async_copy(g_ref, mid.at[pl.ds(1, ROWS)], load_sem.at[0])
    w_load = pltpu.make_async_copy(w2_ref, wbuf, load_sem.at[1])
    a_load = pltpu.make_async_copy(a_ref, sh.at[0, pl.ds(0, ROWS)], load_sem.at[2])
    a_load.start()

    @pl.when(row == 0)
    def _():
        mid[0] = jnp.zeros((COLS, CH), BF16)
        dc[0] = jnp.zeros((COLS, CH), BF16)

    @pl.when(row == n_row - 1)
    def _():
        mid[ROWS + 1] = jnp.zeros((COLS, CH), BF16)
        dc[ROWS + 1] = jnp.zeros((COLS, CH), BF16)

    @pl.when(col == 0)
    def _():
        for u in range(2):
            edge_in[u, 0] = jnp.zeros((32, CH), F32)

    @pl.when(col == n_col - 1)
    def _():
        for u in range(2):
            edge_in[u, 1] = jnp.zeros((32, CH), F32)

    for v in range(2):
        edge_out[v, 24:32] = jnp.zeros((8, CH), F32)

    centers = (mid, dc)

    def row_copy(u, down):
        src_row, dst_row = (ROWS, 0) if down else (1, ROWS + 1)
        dev = {"row": row + 1, "col": col} if down else {"row": row - 1, "col": col}
        n = u * 4 + (0 if down else 1)
        source = dc.at[src_row] if u else g_ref.at[src_row - 1]
        return pltpu.make_async_remote_copy(source, centers[u].at[dst_row], hs_sem.at[n], hr_sem.at[n], device_id=dev, device_id_type=MESH)

    def col_copy(u, right):
        dev = {"row": row, "col": col + 1} if right else {"row": row, "col": col - 1}
        n = u * 4 + (2 if right else 3)
        a, b = (1, 0) if right else (0, 1)
        return pltpu.make_async_remote_copy(edge_out.at[a], edge_in.at[u, b], hs_sem.at[n], hr_sem.at[n], device_id=dev, device_id_type=MESH)

    def send_rows(u):
        @pl.when(row < n_row - 1)
        def _():
            row_copy(u, True).start()

        @pl.when(row > 0)
        def _():
            row_copy(u, False).start()

    def wait_rows(u):
        @pl.when(row > 0)
        def _():
            row_copy(u, True).wait_recv()
            row_copy(u, False).wait_send()

        @pl.when(row < n_row - 1)
        def _():
            row_copy(u, False).wait_recv()
            row_copy(u, True).wait_send()

    def send_cols(u):
        def body(r, _):
            edge_out[0, pl.ds(r, 1)] = centers[u][r, 0:16].astype(F32)[0:1]
            edge_out[1, pl.ds(r, 1)] = centers[u][r, COLS - 16:COLS].astype(F32)[15:16]
            return 0

        lax.fori_loop(0, ROWS + 2, body, 0)

        @pl.when(col < n_col - 1)
        def _():
            col_copy(u, True).start()

        @pl.when(col > 0)
        def _():
            col_copy(u, False).start()

    def wait_cols(u):
        @pl.when(col > 0)
        def _():
            col_copy(u, True).wait_recv()
            col_copy(u, False).wait_send()

        @pl.when(col < n_col - 1)
        def _():
            col_copy(u, False).wait_recv()
            col_copy(u, True).wait_send()

    def build_shift(u, right):
        spot = lax.broadcasted_iota(jnp.int32, (COLS, CH), 0)

        def body(r, _):
            val = centers[u][r].astype(F32)
            edge = edge_in[u, right, pl.ds(r, 1)]
            moved = jnp.where(spot == (COLS - 1 if right else 0), edge, pltpu.roll(val, COLS - 1 if right else 1, 0))
            sh[right, r] = moved.astype(BF16)
            return 0

        with mark("shift"):
            lax.fori_loop(0, ROWS + 2, body, 0)

    def base_of(rot, level):
        off = 0
        for n in range(level):
            off = off + bits[(rot + n) % 3] * HALVES[n + 1]
        return off

    def axis_of(rot, level):
        return mate if level == 0 else flip[(rot + level - 1) % 3]

    def reduce_copy(t, j, level):
        size, cols = HALVES[level], pl.ds(j * WIDTH, WIDTH)
        if level == 0:
            source = part.at[9 + t % 2, :, cols]
            dev = mate
        else:
            rot = t + j
            off = base_of(rot, level - 1) + (1 - bits[(rot + level - 1) % 3]) * size
            source = part.at[t, pl.ds(pl.multiple_of(off, 32), size), cols]
            dev = axis_of(rot, level)
        return pltpu.make_async_remote_copy(source, halves[level].at[t, :, cols], send_sem.at[t, j, level], recv_sem.at[t, j, level], device_id=dev, device_id_type=MESH)

    def gather_copy(w, t, j, level):
        rot = t + j
        off = core * 256 + base_of(rot, level)
        view = full[w].at[ORDER[t], pl.ds(pl.multiple_of(off, 32), HALVES[level]), pl.ds(j * WIDTH, WIDTH)]
        n = 7 - level
        return pltpu.make_async_remote_copy(view, view, send_sem.at[t, j, n], recv_sem.at[t, j, n], device_id=axis_of(rot, level), device_id_type=MESH)

    def event(w, t, j, s):
        if s <= 3:
            reduce_copy(t, j, s).wait_recv()
            cols = slice(j * WIDTH, (j + 1) * WIDTH)
            off = base_of(t + j, s)
            rows = pl.ds(pl.multiple_of(off, 32), HALVES[s]) if s else slice(0, 256)
            total = part[t, rows, cols] + halves[s][t, :, cols]
            if s < 3:
                part[t, rows, cols] = total
                reduce_copy(t, j, s + 1).start()
            else:
                full[w][ORDER[t], pl.ds(pl.multiple_of(core * 256 + off, 32), HALVES[3]), cols] = total
                gather_copy(w, t, j, 3).start()
        else:
            gather_copy(w, t, j, 7 - s).wait_recv()
            if s < 7:
                gather_copy(w, t, j, 6 - s).start()
            else:
                for level in range(4):
                    if level:
                        reduce_copy(t, j, level).wait_send()
                    gather_copy(w, t, j, level).wait_send()

    def pump(n, base, lo, hi):
        if not any(slots[base + m] for m in range(lo, hi)):
            return
        if hi - lo == 1:
            for key in slots[base + lo]:
                event(*key)
            return
        half = (lo + hi) // 2

        @pl.when(n < half)
        def _():
            pump(n, base, lo, half)

        @pl.when(n >= half)
        def _():
            pump(n, base, half, hi)

    def tap_half(n, place, row_at, plane):
        second = n % 2
        rows = pl.ds(pl.multiple_of(core * 256 + (1 - second) * (1 - 2 * core) * 256, 256), 256)

        @pl.when((second == 0) & (place >= 2))
        def _():
            for j in range(PARTS):
                reduce_copy(place - 2, j, 0).wait_send()

        grad = plane[pl.ds(row_at, ROWS)].reshape(PIX, CH)
        part[second * place + (1 - second) * (9 + place % 2)] = lax.dot_general(lv[:, rows], grad, (((0,), (0,)), ((), ())), preferred_element_type=F32)

        @pl.when(second == 0)
        def _():
            for j in range(PARTS):
                reduce_copy(place, j, 0).start()

    def last_sends():
        for t in (7, 8):
            for j in range(PARTS):
                reduce_copy(t, j, 0).wait_send()

    def tap_loops(u, base):
        def middle(n, _):
            if u == 0:
                @pl.when(n < 2)
                def _():
                    with mark("gelu"):
                        gelu_half(n)

                @pl.when(n == 0)
                def _():
                    with mark("barrier"):
                        pl.semaphore_wait(barrier, 8 - row // 3 - (3 - row) // 3 - col // 3 - (3 - col) // 3)
                        send_rows(0)
                        g_load.wait()
                        w_load.start()
                        stage_copy(0, 0).start()

                @pl.when(n == 2)
                def _():
                    with mark("rows"):
                        wait_rows(0)
                        send_cols(0)

            row_at = (n // 2 + 1) % 3
            with mark("center"):
                tap_half(n, n // 2, row_at, centers[u])
            with mark("pump"):
                pump(n, base, 0, 6)
            return 0

        def side(n, _):
            @pl.when(n == 0)
            def _():
                with mark("cols"):
                    wait_cols(u)
                build_shift(u, 1)

            @pl.when(n == 6)
            def _():
                build_shift(u, 0)

            which = n // 6
            row_at = (n // 2 % 3 + 1) % 3
            with mark("side"):
                tap_half(n, 3 + n // 2, row_at, sh.at[1 - which])
            with mark("pump"):
                pump(n, base + 6, 0, 12)
            return 0

        lax.fori_loop(0, 6, middle, 0)
        lax.fori_loop(0, 12, side, 0)

    def conv_rows(g, center):
        lhs = []
        rhs = []
        for k in range(9):
            a, c = k // 3, k % 3
            plane = (sh.at[1], center, sh.at[0])[c]
            lhs.append(plane[pl.ds(g * GROUP + 2 - a, GROUP)].reshape(GPIX, CH))
            rhs.append(wbuf[k])
        return lax.dot_general(jnp.concatenate(lhs, axis=1), jnp.concatenate(rhs, axis=1), (((1,), (1,)), ((), ())), preferred_element_type=F32)

    def group_of(gi):
        return jnp.where(gi == 0, 0, jnp.where(gi == 1, NGROUP - 1, gi - 1))

    def stage_copy(gi, slot):
        return pltpu.make_async_copy(a_ref.at[pl.ds(group_of(gi) * GROUP, GROUP)], stage.at[slot], stage_sem.at[slot])

    def slope_rows(gi, slot):
        a_val = stage[slot].reshape(GPIX, CH).astype(F32)
        d_a = (dzs[...] * gelu_slope(a_val)).astype(BF16)
        dc[pl.ds(group_of(gi) * GROUP + 1, GROUP)] = d_a.reshape(GROUP, COLS, CH)

    def gelu_half(second):
        chans = pl.ds(pl.multiple_of(core * 256 + (1 - second) * (1 - 2 * core) * 256, 256), 256)

        def gelu_row(r, _):
            lv[pl.ds(pl.multiple_of(r * COLS, COLS), COLS), chans] = gelu_val(sh[0, r, :, chans].astype(F32)).astype(BF16)
            return 0

        lax.fori_loop(0, ROWS, gelu_row, 0)

    with mark("aload"):
        a_load.wait()
    g_load.start()
    dzs[...] = jnp.zeros((GPIX, CH), F32)

    tap_loops(0, 0)

    x_load = pltpu.make_async_copy(x_ref, lv, load_sem.at[0])
    x_load.start()
    w_load.wait()

    stage_copy(0, 0).wait()

    def dz_step(gi, _):
        before = jnp.maximum(gi - 1, 0)
        slot = before % 2

        @pl.when(gi >= 2)
        def _():
            stage_copy(before, slot).wait()

        @pl.when(gi >= 1)
        def _():
            stage_copy(gi, gi % 2).start()

        with mark("dz"):
            slope_rows(before, slot)
            dzs[...] = conv_rows(group_of(gi), mid)

        @pl.when(gi == 2)
        def _():
            send_rows(1)

        with mark("pump"):
            pump(gi, 18, 0, NGROUP)
        return 0

    lax.fori_loop(0, NGROUP, dz_step, 0)
    w1_load = pltpu.make_async_copy(w1_ref, wbuf, load_sem.at[1])
    w1_load.start()
    last_sends()
    with mark("between"):
        stage_copy(NGROUP - 1, (NGROUP - 1) % 2).wait()
        slope_rows(NGROUP - 1, (NGROUP - 1) % 2)
        wait_rows(1)
        send_cols(1)
        x_load.wait()

    tap_loops(1, 18 + NGROUP)

    w1_load.wait()

    def dx_step(g, _):
        with mark("dx"):
            val = conv_rows(g, dc) + mid[pl.ds(g * GROUP + 1, GROUP)].reshape(GPIX, CH).astype(F32)
            lv[pl.ds(pl.multiple_of(g * GPIX, GPIX), GPIX)] = val.astype(BF16)
        with mark("pump"):
            pump(g, 36 + NGROUP, 0, NGROUP)
        return 0

    lax.fori_loop(0, NGROUP, dx_step, 0)
    last_sends()
    for key in slots[36 + 2 * NGROUP]:
        with mark("e%d%d%d%d" % key):
            event(*key)


def write_out(lv, full_one, full_two, dx_ref, dw1_ref, dw2_ref, sem):
    copies = [pltpu.make_async_copy(lv.at[pl.ds(k * 512, 512)], dx_ref.at[pl.ds(k * 512, 512)], sem.at[k]) for k in range(9)]
    copies += [pltpu.make_async_copy(full_one.at[k], dw1_ref.at[k], sem.at[9 + k]) for k in range(9)]
    copies += [pltpu.make_async_copy(full_two.at[k], dw2_ref.at[k], sem.at[18 + k]) for k in range(9)]
    for copy in copies:
        copy.start()
    for copy in copies:
        copy.wait()


def solution(mesh):
    slots, _ = build_slots((3, 0, 2, 0, 3, 3, 0, 3), (2, 3, 0, 0, 2, 0, 2, 2))
    any_spec = pl.BlockSpec(memory_space=pl.ANY)
    vmem_spec = pl.BlockSpec(memory_space=pltpu.VMEM)

    def local_step(x_tile, a_tile, g_tile, w_one, w_two):
        lv, full_one, full_two = pl.pallas_call(
            functools.partial(kernel, slots),
            out_shape=(pltpu.VMEM((PIX, CH), BF16), pltpu.VMEM((9, CH, CH), F32), pltpu.VMEM((9, CH, CH), F32)),
            in_specs=[any_spec] * 5,
            out_specs=[vmem_spec] * 3,
            scratch_shapes=[
                pltpu.VMEM((11, 256, CH), F32),
                pltpu.VMEM((9, 256, CH), F32),
                pltpu.VMEM((9, 128, CH), F32),
                pltpu.VMEM((9, 64, CH), F32),
                pltpu.VMEM((9, 32, CH), F32),
                pltpu.VMEM((ROWS + 2, COLS, CH), BF16),
                pltpu.VMEM((ROWS + 2, COLS, CH), BF16),
                pltpu.VMEM((2, ROWS + 2, COLS, CH), BF16),
                pltpu.VMEM((9, CH, CH), BF16),
                pltpu.VMEM((2, GROUP, COLS, CH), BF16),
                pltpu.VMEM((2, 32, CH), F32),
                pltpu.VMEM((2, 2, 32, CH), F32),
                pltpu.SemaphoreType.DMA((9, PARTS, 8)),
                pltpu.SemaphoreType.DMA((9, PARTS, 8)),
                pltpu.SemaphoreType.DMA((8,)),
                pltpu.SemaphoreType.DMA((8,)),
                pltpu.SemaphoreType.DMA((3,)),
                pltpu.SemaphoreType.DMA((2,)),
            ],
            compiler_params=pltpu.CompilerParams(collective_id=0, has_side_effects=True, vmem_limit_bytes=43440000),
        )(x_tile.reshape(PIX, CH), a_tile.reshape(ROWS, COLS, CH), g_tile.reshape(ROWS, COLS, CH), w_one.reshape(9, CH, CH), w_two.reshape(9, CH, CH))
        d_x, d_w1, d_w2 = pl.pallas_call(
            write_out,
            out_shape=(jax.ShapeDtypeStruct((PIX, CH), BF16), jax.ShapeDtypeStruct((9, CH, CH), F32), jax.ShapeDtypeStruct((9, CH, CH), F32)),
            in_specs=[vmem_spec] * 3,
            out_specs=[any_spec] * 3,
            scratch_shapes=[pltpu.SemaphoreType.DMA((27,))],
            compiler_params=pltpu.CompilerParams(vmem_limit_bytes=4000000),
        )(lv, full_one, full_two)
        return d_x.reshape(1, ROWS, COLS, CH), d_w1.reshape(3, 3, CH, CH), d_w2.reshape(3, 3, CH, CH)

    tile_spec = P(None, "row", "col", None)
    return jax.shard_map(local_step, mesh=mesh, in_specs=(tile_spec, tile_spec, tile_spec, P(), P()), out_specs=(tile_spec, P(), P()), check_vma=False)
```

```python
import functools

import jax
import jax.numpy as jnp
from jax import lax
from jax.experimental import pallas as pl
from jax.experimental.pallas import tpu as pltpu
from jax.sharding import PartitionSpec as P

MESH = pl.DeviceIdType.MESH
F32 = jnp.float32
BF16 = jnp.bfloat16
mark = jax.named_scope
ROWS, COLS, CH = 24, 192, 512
PIX = ROWS * COLS
GROUP = 2
GPIX = GROUP * COLS
NGROUP = ROWS // GROUP
HALVES = (256, 128, 64, 32)
PARTS = 2
WIDTH = CH // PARTS
SIDE = 256
ORDER = (4, 1, 7, 3, 0, 6, 5, 2, 8)


def step_lengths():
    steps = []
    for w in range(2):
        extra = {0: 2.4, 1: 1.7, 6: 1.3, 12: 1.3} if w == 0 else {0: 0.75, 6: 1.3, 12: 1.3}
        steps += [(1.48 + extra.get(n, 0.0), (w, n)) for n in range(18)]
        steps += [((2.08 if w else 2.35), None)] * NGROUP
    return steps


def build_slots(rank=(0, 1, 2, 3, 4, 5, 6, 7), tail_rank=(0, 1, 2, 3, 4, 5, 6, 7), first=8.8, rate=46.6, lat=2.3, hop=1.8, slack=0.0):
    size = {1: 0.262144e3, 2: 0.131072e3, 3: 0.065536e3}
    add = (0.075, 0.04, 0.02, 0.01)
    link = [0.0, 0.0, 0.0]
    arrive = {}

    def send(now, w, t, j, s):
        if s in (0, 7):
            arrive[(w, t, j, s)] = now + hop * (0.6 + 0.4 / PARTS)
            return
        level = s if s <= 3 else 7 - s
        axis = (t + j + level - 1) % 3
        link[axis] = max(now, link[axis]) + size[level] / PARTS / rate
        arrive[(w, t, j, s)] = link[axis] + lat

    def handle(now, key):
        del arrive[key]
        w, t, j, s = key
        now += 0.03 + (add[s] / PARTS if s < 4 else 0.0)
        if s < 7:
            send(now, w, t, j, s + 1)
        return now

    now = first
    slots = []
    for length, made in step_lengths():
        if made is not None and made[0] == 1 and made[1] % 2 == 0:
            while any(k[0] == 0 and k[1] == made[1] // 2 for k in arrive):
                when, key = min((v, k) for k, v in arrive.items())
                now = handle(max(now, when), key)
                slots[-1].append(key)
        now += length
        fresh = None
        if made is not None and made[1] % 2 == 0:
            fresh = (made[0], made[1] // 2)
            for j in range(PARTS):
                send(now + 0.1, made[0], made[1] // 2, j, 0)
        here = []
        while True:
            ready = [(rank[k[3]], v, k) for k, v in arrive.items() if v + slack <= now and not (k[3] == 0 and k[:2] == fresh)]
            if not ready:
                break
            key = min(ready)[2]
            now = handle(now, key)
            here.append(key)
        slots.append(here)
    tail = []
    while arrive:
        now = max(now, min(arrive.values()))
        key = min((tail_rank[k[3]], v, k) for k, v in arrive.items() if v <= now)[2]
        now = handle(now, key)
        tail.append(key)
    slots.append(tail)
    return slots, now


def gate(a):
    w = (0.044715 * 0.7978845608028654) * (a * a)
    return 0.5 * jnp.tanh(a * (0.7978845608028654 + w)) + 0.5, w


def gelu_val(a):
    return a * gate(a)[0]


def gelu_slope(a):
    p, w = gate(a)
    return p + (a * p) * ((1.0 - p) * (2.0 * 0.7978845608028654 + 6.0 * w))


def kernel(slots, x_ref, a_ref, g_ref, w1_ref, w2_ref, lv, full_one, full_two,
           part, r0, r1, r2, r3, mid, dc, sh, wbuf, stage, edge_in, corner_out,
           send_sem, recv_sem, hs_sem, hr_sem, load_sem, stage_sem):
    row = lax.axis_index("row")
    col = lax.axis_index("col")
    n_row, n_col = 4, 4
    core = row % 2
    bits = (row // 2, col % 2, col // 2)
    flip = ({"row": row + 2 - 4 * (row // 2), "col": col}, {"row": row, "col": col + 1 - 2 * (col % 2)}, {"row": row, "col": col + 2 - 4 * (col // 2)})
    mate = {"row": row + 1 - 2 * core, "col": col}
    halves = (r0, r1, r2, r3)
    full = (full_two, full_one)
    dzs = full_one.at[8, pl.ds(0, GPIX)]

    def edge_out(side):
        return full_one.at[8, pl.ds(GPIX + side * ROWS, ROWS)]

    def corner_in(u, side, end):
        return full_one.at[8, pl.ds(GPIX + 2 * ROWS + 8 * (4 * u + 2 * side + end), 8)]


    barrier = pltpu.get_barrier_semaphore()
    for dev in (mate,) + flip:
        pl.semaphore_signal(barrier, inc=1, device_id=dev, device_id_type=MESH)
    steps = (-1, 0, 1)

    def has(dr, dc_):
        conds = []
        if dr:
            conds.append(row > 0 if dr < 0 else row < n_row - 1)
        if dc_:
            conds.append(col > 0 if dc_ < 0 else col < n_col - 1)
        return conds[0] if len(conds) == 1 else conds[0] & conds[1]

    near = [(dr, dk) for dr in steps for dk in steps if dr or dk]
    for dr, dk in near:
        @pl.when(has(dr, dk))
        def _():
            pl.semaphore_signal(barrier, inc=1, device_id={"row": row + dr, "col": col + dk}, device_id_type=MESH)
    near_count = (3 - row // 3 - (3 - row) // 3) * (3 - col // 3 - (3 - col) // 3) - 1

    g_load = pltpu.make_async_copy(g_ref, mid.at[pl.ds(1, ROWS)], load_sem.at[0])
    w_load = pltpu.make_async_copy(w2_ref, wbuf, load_sem.at[1])
    third = ROWS // 3
    a_loads = [pltpu.make_async_copy(a_ref.at[pl.ds(n * third, third)], sh.at[0, pl.ds(n * third, third)], load_sem.at[2 + n]) for n in range(3)]
    for copy in a_loads:
        copy.start()

    @pl.when(row == 0)
    def _():
        mid[0] = jnp.zeros((COLS, CH), BF16)
        dc[0] = jnp.zeros((COLS, CH), BF16)

    @pl.when(row == n_row - 1)
    def _():
        mid[ROWS + 1] = jnp.zeros((COLS, CH), BF16)
        dc[ROWS + 1] = jnp.zeros((COLS, CH), BF16)

    for u in range(2):
        for side in range(2):
            @pl.when(col == (0, n_col - 1)[side])
            def _():
                edge_in[u, side] = jnp.zeros((ROWS, CH), F32)

            for end in range(2):
                @pl.when((col == (0, n_col - 1)[side]) | (row == (0, n_row - 1)[end]))
                def _():
                    corner_in(u, side, end)[...] = jnp.zeros((8, CH), F32)

    centers = (mid, dc)

    def row_copy(u, down):
        src_row, dst_row = (ROWS, 0) if down else (1, ROWS + 1)
        dev = {"row": row + 1, "col": col} if down else {"row": row - 1, "col": col}
        n = u * 4 + (0 if down else 1)
        source = dc.at[src_row] if u else g_ref.at[src_row - 1]
        return pltpu.make_async_remote_copy(source, centers[u].at[dst_row], hs_sem.at[n], hr_sem.at[n], device_id=dev, device_id_type=MESH)

    def col_copy(u, right):
        n = u * 4 + (2 if right else 3)
        a, b = (1, 0) if right else (0, 1)
        return pltpu.make_async_remote_copy(edge_out(a), edge_in.at[u, b], hs_sem.at[n], hr_sem.at[n], device_id={"row": row, "col": col + 2 * right - 1}, device_id_type=MESH)

    def corner_copy(u, right, down):
        n = 8 + u * 4 + 2 * right + down
        return pltpu.make_async_remote_copy(corner_out.at[right, down], corner_in(u, 1 - right, 1 - down), hs_sem.at[n], hr_sem.at[n], device_id={"row": row + 2 * down - 1, "col": col + 2 * right - 1}, device_id_type=MESH)

    def send_rows(u):
        @pl.when(row < n_row - 1)
        def _():
            row_copy(u, True).start()

        @pl.when(row > 0)
        def _():
            row_copy(u, False).start()

    def wait_rows(u):
        @pl.when(row > 0)
        def _():
            row_copy(u, True).wait_recv()
            row_copy(u, False).wait_send()

        @pl.when(row < n_row - 1)
        def _():
            row_copy(u, False).wait_recv()
            row_copy(u, True).wait_send()

    def edge_of(u, r, right):
        if right:
            return centers[u][r, COLS - 16:COLS].astype(F32)[15:16]
        return centers[u][r, 0:16].astype(F32)[0:1]

    def send_cols(u):
        def body(r, _):
            for side in range(2):
                edge_out(side)[pl.ds(r, 1)] = edge_of(u, r + 1, side)
            return 0

        lax.fori_loop(0, ROWS, body, 0)
        for right in range(2):
            for down in range(2):
                corner_out[right, down] = jnp.broadcast_to(edge_of(u, ROWS if down else 1, right), (8, CH))
        for right in range(2):
            @pl.when(has(0, 2 * right - 1))
            def _():
                col_copy(u, right).start()

            for down in range(2):
                @pl.when(has(2 * down - 1, 2 * right - 1))
                def _():
                    corner_copy(u, right, down).start()

    def wait_cols(u):
        for right in range(2):
            @pl.when(has(0, 2 * right - 1))
            def _():
                col_copy(u, 1 - right).wait_recv()
                col_copy(u, right).wait_send()

            for down in range(2):
                @pl.when(has(2 * down - 1, 2 * right - 1))
                def _():
                    corner_copy(u, 1 - right, 1 - down).wait_recv()
                    corner_copy(u, right, down).wait_send()

    def build_shift(u, right):
        spot = lax.broadcasted_iota(jnp.int32, (COLS, CH), 0)

        def fill(r, edge):
            val = centers[u][r].astype(F32)
            moved = jnp.where(spot == (COLS - 1 if right else 0), edge, pltpu.roll(val, COLS - 1 if right else 1, 0))
            sh[right, r] = moved.astype(BF16)

        def body(r, _):
            fill(r + 1, edge_in[u, right, pl.ds(r, 1)])
            return 0

        with mark("shift"):
            lax.fori_loop(0, ROWS, body, 0)
            for end in range(2):
                fill(end * (ROWS + 1), corner_in(u, right, end)[0:1])

    def base_of(rot, level):
        off = 0
        for n in range(level):
            off = off + bits[(rot + n) % 3] * HALVES[n + 1]
        return off

    def axis_of(rot, level):
        return mate if level == 0 else flip[(rot + level - 1) % 3]

    def reduce_copy(t, j, level):
        size, cols = HALVES[level], pl.ds(j * WIDTH, WIDTH)
        if level == 0:
            source = part.at[9 + t % 2, :, cols]
            dev = mate
        else:
            rot = t + j
            off = base_of(rot, level - 1) + (1 - bits[(rot + level - 1) % 3]) * size
            source = part.at[t, pl.ds(pl.multiple_of(off, 32), size), cols]
            dev = axis_of(rot, level)
        return pltpu.make_async_remote_copy(source, halves[level].at[t, :, cols], send_sem.at[t, j, level], recv_sem.at[t, j, level], device_id=dev, device_id_type=MESH)

    def gather_copy(w, t, j, level):
        rot = t + j
        off = core * 256 + base_of(rot, level)
        view = full[w].at[ORDER[t], pl.ds(pl.multiple_of(off, 32), HALVES[level]), pl.ds(j * WIDTH, WIDTH)]
        n = 7 - level
        return pltpu.make_async_remote_copy(view, view, send_sem.at[t, j, n], recv_sem.at[t, j, n], device_id=axis_of(rot, level), device_id_type=MESH)

    def event(w, t, j, s):
        if s <= 3:
            reduce_copy(t, j, s).wait_recv()
            cols = slice(j * WIDTH, (j + 1) * WIDTH)
            off = base_of(t + j, s)
            rows = pl.ds(pl.multiple_of(off, 32), HALVES[s]) if s else slice(0, 256)
            total = part[t, rows, cols] + halves[s][t, :, cols]
            if s < 3:
                part[t, rows, cols] = total
                reduce_copy(t, j, s + 1).start()
            else:
                full[w][ORDER[t], pl.ds(pl.multiple_of(core * 256 + off, 32), HALVES[3]), cols] = total
                gather_copy(w, t, j, 3).start()
        else:
            gather_copy(w, t, j, 7 - s).wait_recv()
            if s < 7:
                gather_copy(w, t, j, 6 - s).start()
            else:
                for level in range(4):
                    if level:
                        reduce_copy(t, j, level).wait_send()
                    gather_copy(w, t, j, level).wait_send()

    def pump(n, base, lo, hi):
        if not any(slots[base + m] for m in range(lo, hi)):
            return
        if hi - lo == 1:
            for key in slots[base + lo]:
                event(*key)
            return
        half = (lo + hi) // 2

        @pl.when(n < half)
        def _():
            pump(n, base, lo, half)

        @pl.when(n >= half)
        def _():
            pump(n, base, half, hi)

    def tap_half(n, place, row_at, plane):
        second = n % 2
        rows = pl.ds(pl.multiple_of(core * 256 + (1 - second) * (1 - 2 * core) * 256, 256), 256)

        @pl.when((second == 0) & (place >= 2))
        def _():
            for j in range(PARTS):
                reduce_copy(place - 2, j, 0).wait_send()

        grad = plane[pl.ds(row_at, ROWS)].reshape(PIX, CH)
        part[second * place + (1 - second) * (9 + place % 2)] = lax.dot_general(lv[:, rows], grad, (((0,), (0,)), ((), ())), preferred_element_type=F32)

        @pl.when(second == 0)
        def _():
            for j in range(PARTS):
                reduce_copy(place, j, 0).start()

    def last_sends():
        for t in (7, 8):
            for j in range(PARTS):
                reduce_copy(t, j, 0).wait_send()

    def tap_loops(u, base):
        def middle(n, _):
            if u == 0:
                @pl.when(n == 1)
                def _():
                    with mark("gelu"):
                        gelu_half(1, False)

                @pl.when(n == 0)
                def _():
                    with mark("gelu"):
                        gelu_half(0, True)
                    with mark("barrier"):
                        pl.semaphore_wait(barrier, 4 + near_count)
                        send_rows(0)
                        g_load.wait()
                        send_cols(0)
                        w_load.start()
                        stage_copy(0, 0).start()

            @pl.when(n == 2)
            def _():
                with mark("rows"):
                    wait_rows(u)

            row_at = (n // 2 + 1) % 3
            with mark("center"):
                tap_half(n, n // 2, row_at, centers[u])
            with mark("pump"):
                pump(n, base, 0, 6)
            return 0

        def side(n, _):
            @pl.when(n == 0)
            def _():
                with mark("cols"):
                    wait_cols(u)
                build_shift(u, 1)

            @pl.when(n == 6)
            def _():
                build_shift(u, 0)

            which = n // 6
            row_at = (n // 2 % 3 + 1) % 3
            with mark("side"):
                tap_half(n, 3 + n // 2, row_at, sh.at[1 - which])
            with mark("pump"):
                pump(n, base + 6, 0, 12)
            return 0

        lax.fori_loop(0, 6, middle, 0)
        lax.fori_loop(0, 12, side, 0)

    def conv_rows(g, center):
        lhs = []
        rhs = []
        for k in range(9):
            a, c = k // 3, k % 3
            plane = (sh.at[1], center, sh.at[0])[c]
            lhs.append(plane[pl.ds(g * GROUP + 2 - a, GROUP)].reshape(GPIX, CH))
            rhs.append(wbuf[k])
        return lax.dot_general(jnp.concatenate(lhs, axis=1), jnp.concatenate(rhs, axis=1), (((1,), (1,)), ((), ())), preferred_element_type=F32)

    def group_of(gi):
        return jnp.where(gi == 0, 0, jnp.where(gi == 1, NGROUP - 1, gi - 1))

    def stage_copy(gi, slot):
        return pltpu.make_async_copy(a_ref.at[pl.ds(group_of(gi) * GROUP, GROUP)], stage.at[slot], stage_sem.at[slot])

    def slope_rows(gi, slot):
        a_val = stage[slot].reshape(GPIX, CH).astype(F32)
        d_a = (dzs[...] * gelu_slope(a_val)).astype(BF16)
        dc[pl.ds(group_of(gi) * GROUP + 1, GROUP)] = d_a.reshape(GROUP, COLS, CH)

    def gelu_half(second, first):
        chans = pl.ds(pl.multiple_of(core * 256 + (1 - second) * (1 - 2 * core) * 256, 256), 256)

        def gelu_row(r, _):
            lv[pl.ds(pl.multiple_of(r * COLS, COLS), COLS), chans] = gelu_val(sh[0, r, :, chans].astype(F32)).astype(BF16)
            return 0

        for part_n in range(3):
            if first:
                a_loads[part_n].wait()
            lax.fori_loop(part_n * third, (part_n + 1) * third, gelu_row, 0)

    g_load.start()
    dzs[...] = jnp.zeros((GPIX, CH), F32)

    tap_loops(0, 0)

    x_load = pltpu.make_async_copy(x_ref, lv, load_sem.at[0])
    x_load.start()
    w_load.wait()

    stage_copy(0, 0).wait()

    def dz_step(gi, _):
        before = jnp.maximum(gi - 1, 0)
        slot = before % 2

        @pl.when(gi >= 2)
        def _():
            stage_copy(before, slot).wait()

        @pl.when(gi >= 1)
        def _():
            stage_copy(gi, gi % 2).start()

        with mark("dz"):
            slope_rows(before, slot)
            dzs[...] = conv_rows(group_of(gi), mid)

        @pl.when(gi == 2)
        def _():
            send_rows(1)

        with mark("pump"):
            pump(gi, 18, 0, NGROUP)
        return 0

    lax.fori_loop(0, NGROUP, dz_step, 0)
    w1_load = pltpu.make_async_copy(w1_ref, wbuf, load_sem.at[1])
    w1_load.start()
    last_sends()
    with mark("between"):
        stage_copy(NGROUP - 1, (NGROUP - 1) % 2).wait()
        slope_rows(NGROUP - 1, (NGROUP - 1) % 2)
        send_cols(1)
        x_load.wait()

    tap_loops(1, 18 + NGROUP)

    w1_load.wait()

    def dx_step(g, _):
        with mark("dx"):
            val = conv_rows(g, dc) + mid[pl.ds(g * GROUP + 1, GROUP)].reshape(GPIX, CH).astype(F32)
            lv[pl.ds(pl.multiple_of(g * GPIX, GPIX), GPIX)] = val.astype(BF16)
        with mark("pump"):
            pump(g, 36 + NGROUP, 0, NGROUP)
        return 0

    lax.fori_loop(0, NGROUP, dx_step, 0)
    last_sends()
    for key in slots[36 + 2 * NGROUP]:
        with mark("e%d%d%d%d" % key):
            event(*key)


def write_out(lv, full_one, full_two, dx_ref, dw1_ref, dw2_ref, sem):
    copies = [pltpu.make_async_copy(lv.at[pl.ds(k * 512, 512)], dx_ref.at[pl.ds(k * 512, 512)], sem.at[k]) for k in range(9)]
    copies += [pltpu.make_async_copy(full_one.at[k], dw1_ref.at[k], sem.at[9 + k]) for k in range(9)]
    copies += [pltpu.make_async_copy(full_two.at[k], dw2_ref.at[k], sem.at[18 + k]) for k in range(9)]
    for copy in copies:
        copy.start()
    for copy in copies:
        copy.wait()


def solution(mesh):
    slots, _ = build_slots((0, 1, 1, 2, 3, 2, 3, 1), (3, 0, 1, 0, 3, 0, 3, 1), slack=0.3)
    any_spec = pl.BlockSpec(memory_space=pl.ANY)
    vmem_spec = pl.BlockSpec(memory_space=pltpu.VMEM)

    def local_step(x_tile, a_tile, g_tile, w_one, w_two):
        lv, full_one, full_two = pl.pallas_call(
            functools.partial(kernel, slots),
            out_shape=(pltpu.VMEM((PIX, CH), BF16), pltpu.VMEM((9, CH, CH), F32), pltpu.VMEM((9, CH, CH), F32)),
            in_specs=[any_spec] * 5,
            out_specs=[vmem_spec] * 3,
            scratch_shapes=[
                pltpu.VMEM((11, 256, CH), F32),
                pltpu.VMEM((9, 256, CH), F32),
                pltpu.VMEM((9, 128, CH), F32),
                pltpu.VMEM((9, 64, CH), F32),
                pltpu.VMEM((9, 32, CH), F32),
                pltpu.VMEM((ROWS + 2, COLS, CH), BF16),
                pltpu.VMEM((ROWS + 2, COLS, CH), BF16),
                pltpu.VMEM((2, ROWS + 2, COLS, CH), BF16),
                pltpu.VMEM((9, CH, CH), BF16),
                pltpu.VMEM((2, GROUP, COLS, CH), BF16),
                pltpu.VMEM((2, 2, ROWS, CH), F32),
                pltpu.VMEM((2, 2, 8, CH), F32),
                pltpu.SemaphoreType.DMA((9, PARTS, 8)),
                pltpu.SemaphoreType.DMA((9, PARTS, 8)),
                pltpu.SemaphoreType.DMA((16,)),
                pltpu.SemaphoreType.DMA((16,)),
                pltpu.SemaphoreType.DMA((5,)),
                pltpu.SemaphoreType.DMA((2,)),
            ],
            compiler_params=pltpu.CompilerParams(collective_id=0, has_side_effects=True, vmem_limit_bytes=43440000),
        )(x_tile.reshape(PIX, CH), a_tile.reshape(ROWS, COLS, CH), g_tile.reshape(ROWS, COLS, CH), w_one.reshape(9, CH, CH), w_two.reshape(9, CH, CH))
        d_x, d_w1, d_w2 = pl.pallas_call(
            write_out,
            out_shape=(jax.ShapeDtypeStruct((PIX, CH), BF16), jax.ShapeDtypeStruct((9, CH, CH), F32), jax.ShapeDtypeStruct((9, CH, CH), F32)),
            in_specs=[vmem_spec] * 3,
            out_specs=[any_spec] * 3,
            scratch_shapes=[pltpu.SemaphoreType.DMA((27,))],
            compiler_params=pltpu.CompilerParams(vmem_limit_bytes=4000000),
        )(lv, full_one, full_two)
        return d_x.reshape(1, ROWS, COLS, CH), d_w1.reshape(3, 3, CH, CH), d_w2.reshape(3, 3, CH, CH)

    tile_spec = P(None, "row", "col", None)
    return jax.shard_map(local_step, mesh=mesh, in_specs=(tile_spec, tile_spec, tile_spec, P(), P()), out_specs=(tile_spec, P(), P()), check_vma=False)
```

```python
import functools

import jax
import jax.numpy as jnp
from jax import lax
from jax.experimental import pallas as pl
from jax.experimental.pallas import tpu as pltpu
from jax.sharding import PartitionSpec as P

MESH = pl.DeviceIdType.MESH
F32 = jnp.float32
BF16 = jnp.bfloat16
mark = jax.named_scope
ROWS, COLS, CH = 24, 192, 512
PIX = ROWS * COLS
GROUP = 2
GPIX = GROUP * COLS
NGROUP = ROWS // GROUP
HALVES = (256, 128, 64, 32)
PARTS = 2
WIDTH = CH // PARTS
SIDE = 256
ORDER = (4, 1, 7, 3, 0, 6, 5, 2, 8)


def step_lengths():
    steps = []
    for w in range(2):
        extra = {0: 2.5, 1: 1.75, 6: 1.3, 12: 1.3} if w == 0 else {0: 0.75, 6: 1.3, 12: 1.3}
        steps += [(1.48 + extra.get(n, 0.0), (w, n)) for n in range(18)]
        steps += [((2.08 if w else 2.35), None)] * NGROUP
    return steps


def build_slots(rank=(0, 1, 2, 3, 4, 5, 6, 7), tail_rank=(0, 1, 2, 3, 4, 5, 6, 7), first=8.8, rate=46.6, lat=2.45, hop=1.8, slack=0.0):
    size = {1: 0.262144e3, 2: 0.131072e3, 3: 0.065536e3}
    add = (0.075, 0.04, 0.02, 0.01)
    link = [0.0, 0.0, 0.0]
    arrive = {}

    def send(now, w, t, j, s):
        if s in (0, 7):
            arrive[(w, t, j, s)] = now + hop * (0.6 + 0.4 / PARTS)
            return
        level = s if s <= 3 else 7 - s
        axis = (t + j + level - 1) % 3
        link[axis] = max(now, link[axis]) + size[level] / PARTS / rate
        arrive[(w, t, j, s)] = link[axis] + lat

    def handle(now, key):
        del arrive[key]
        w, t, j, s = key
        now += 0.03 + (add[s] / PARTS if s < 4 else 0.0)
        if s < 7:
            send(now, w, t, j, s + 1)
        return now

    now = first
    slots = []
    for length, made in step_lengths():
        if made is not None and made[0] == 1 and made[1] % 2 == 0:
            while any(k[0] == 0 and k[1] == made[1] // 2 for k in arrive):
                when, key = min((v, k) for k, v in arrive.items())
                now = handle(max(now, when), key)
                slots[-1].append(key)
        now += length
        fresh = None
        if made is not None and made[1] % 2 == 0:
            fresh = (made[0], made[1] // 2)
            for j in range(PARTS):
                send(now + 0.1, made[0], made[1] // 2, j, 0)
        here = []
        while True:
            ready = [(rank[k[3]], v, k) for k, v in arrive.items() if v + (3.0 if k[3] == 7 else slack) <= now and k[::3] != (1, 7) and not (k[3] == 0 and k[:2] == fresh)]
            if not ready:
                break
            key = min(ready)[2]
            now = handle(now, key)
            here.append(key)
        slots.append(here)
    tail = []
    while arrive:
        rest = {k: v for k, v in arrive.items() if k[3] != 7} or arrive
        now = max(now, min(rest.values()))
        key = min((tail_rank[k[3]], v, k) for k, v in rest.items() if v <= now)[2]
        now = handle(now, key)
        tail.append(key)
    slots.append(tail)
    return slots, now


def gate(a):
    w = (0.044715 * 0.7978845608028654) * (a * a)
    return 0.5 * jnp.tanh(a * (0.7978845608028654 + w)) + 0.5, w


def gelu_val(a):
    return a * gate(a)[0]


def gelu_slope(a):
    p, w = gate(a)
    return p + (a * p) * ((1.0 - p) * (2.0 * 0.7978845608028654 + 6.0 * w))


def kernel(slots, x_ref, a_ref, g_ref, w1_ref, w2_ref, lv, full_one, full_two,
           part, r0, r1, r2, r3, mid, dc, sh, wbuf, stage, edge_in, corner_out,
           send_sem, give_sem, recv_sem, hs_sem, hr_sem, load_sem, stage_sem):
    row = lax.axis_index("row")
    col = lax.axis_index("col")
    n_row, n_col = 4, 4
    core = row % 2
    bits = (row // 2, col % 2, col // 2)
    flip = ({"row": row + 2 - 4 * (row // 2), "col": col}, {"row": row, "col": col + 1 - 2 * (col % 2)}, {"row": row, "col": col + 2 - 4 * (col // 2)})
    mate = {"row": row + 1 - 2 * core, "col": col}
    halves = (r0, r1, r2, r3)
    full = (full_two, full_one)
    dzs = full_one.at[8, pl.ds(0, GPIX)]

    def edge_out(side):
        return full_one.at[8, pl.ds(GPIX + side * ROWS, ROWS)]

    def corner_in(u, side, end):
        return full_one.at[8, pl.ds(GPIX + 2 * ROWS + 8 * (4 * u + 2 * side + end), 8)]


    barrier = pltpu.get_barrier_semaphore()
    for dev in (mate,) + flip:
        pl.semaphore_signal(barrier, inc=1, device_id=dev, device_id_type=MESH)
    steps = (-1, 0, 1)

    def has(dr, dc_):
        conds = []
        if dr:
            conds.append(row > 0 if dr < 0 else row < n_row - 1)
        if dc_:
            conds.append(col > 0 if dc_ < 0 else col < n_col - 1)
        return conds[0] if len(conds) == 1 else conds[0] & conds[1]

    near = [(dr, dk) for dr in steps for dk in steps if dr or dk]
    for dr, dk in near:
        @pl.when(has(dr, dk))
        def _():
            pl.semaphore_signal(barrier, inc=1, device_id={"row": row + dr, "col": col + dk}, device_id_type=MESH)
    near_count = (3 - row // 3 - (3 - row) // 3) * (3 - col // 3 - (3 - col) // 3) - 1

    g_load = pltpu.make_async_copy(g_ref, mid.at[pl.ds(1, ROWS)], load_sem.at[0])
    w_load = pltpu.make_async_copy(w2_ref, wbuf, load_sem.at[1])
    third = ROWS // 3
    a_loads = [pltpu.make_async_copy(a_ref.at[pl.ds(n * third, third)], sh.at[0, pl.ds(n * third, third)], load_sem.at[2 + n]) for n in range(3)]
    for copy in a_loads:
        copy.start()

    @pl.when(row == 0)
    def _():
        mid[0] = jnp.zeros((COLS, CH), BF16)
        dc[0] = jnp.zeros((COLS, CH), BF16)

    @pl.when(row == n_row - 1)
    def _():
        mid[ROWS + 1] = jnp.zeros((COLS, CH), BF16)
        dc[ROWS + 1] = jnp.zeros((COLS, CH), BF16)

    for u in range(2):
        for side in range(2):
            @pl.when(col == (0, n_col - 1)[side])
            def _():
                edge_in[u, side] = jnp.zeros((ROWS, CH), F32)

            for end in range(2):
                @pl.when((col == (0, n_col - 1)[side]) | (row == (0, n_row - 1)[end]))
                def _():
                    corner_in(u, side, end)[...] = jnp.zeros((8, CH), F32)

    centers = (mid, dc)

    def row_copy(u, down):
        src_row, dst_row = (ROWS, 0) if down else (1, ROWS + 1)
        dev = {"row": row + 1, "col": col} if down else {"row": row - 1, "col": col}
        n = u * 4 + (0 if down else 1)
        source = dc.at[src_row] if u else g_ref.at[src_row - 1]
        return pltpu.make_async_remote_copy(source, centers[u].at[dst_row], hs_sem.at[n], hr_sem.at[n], device_id=dev, device_id_type=MESH)

    def col_copy(u, right):
        n = u * 4 + (2 if right else 3)
        a, b = (1, 0) if right else (0, 1)
        return pltpu.make_async_remote_copy(edge_out(a), edge_in.at[u, b], hs_sem.at[n], hr_sem.at[n], device_id={"row": row, "col": col + 2 * right - 1}, device_id_type=MESH)

    def corner_copy(u, right, down):
        n = 8 + u * 4 + 2 * right + down
        return pltpu.make_async_remote_copy(corner_out.at[right, down], corner_in(u, 1 - right, 1 - down), hs_sem.at[n], hr_sem.at[n], device_id={"row": row + 2 * down - 1, "col": col + 2 * right - 1}, device_id_type=MESH)

    def send_rows(u):
        @pl.when(row < n_row - 1)
        def _():
            row_copy(u, True).start()

        @pl.when(row > 0)
        def _():
            row_copy(u, False).start()

    def wait_rows(u):
        @pl.when(row > 0)
        def _():
            row_copy(u, True).wait_recv()
            row_copy(u, False).wait_send()

        @pl.when(row < n_row - 1)
        def _():
            row_copy(u, False).wait_recv()
            row_copy(u, True).wait_send()

    def edge_of(u, r, right):
        if right:
            return centers[u][r, COLS - 16:COLS].astype(F32)[15:16]
        return centers[u][r, 0:16].astype(F32)[0:1]

    def send_cols(u):
        def body(r, _):
            for side in range(2):
                edge_out(side)[pl.ds(r, 1)] = edge_of(u, r + 1, side)
            return 0

        lax.fori_loop(0, ROWS, body, 0)
        for right in range(2):
            for down in range(2):
                corner_out[right, down] = jnp.broadcast_to(edge_of(u, ROWS if down else 1, right), (8, CH))
        for right in range(2):
            @pl.when(has(0, 2 * right - 1))
            def _():
                col_copy(u, right).start()

            for down in range(2):
                @pl.when(has(2 * down - 1, 2 * right - 1))
                def _():
                    corner_copy(u, right, down).start()

    def wait_cols(u):
        for right in range(2):
            @pl.when(has(0, 2 * right - 1))
            def _():
                col_copy(u, 1 - right).wait_recv()
                col_copy(u, right).wait_send()

            for down in range(2):
                @pl.when(has(2 * down - 1, 2 * right - 1))
                def _():
                    corner_copy(u, 1 - right, 1 - down).wait_recv()
                    corner_copy(u, right, down).wait_send()

    def build_shift(u, right):
        spot = lax.broadcasted_iota(jnp.int32, (COLS, CH), 0)

        def fill(r, edge):
            val = centers[u][r].astype(F32)
            moved = jnp.where(spot == (COLS - 1 if right else 0), edge, pltpu.roll(val, COLS - 1 if right else 1, 0))
            sh[right, r] = moved.astype(BF16)

        def body(r, _):
            fill(r + 1, edge_in[u, right, pl.ds(r, 1)])
            return 0

        with mark("shift"):
            lax.fori_loop(0, ROWS, body, 0)
            for end in range(2):
                fill(end * (ROWS + 1), corner_in(u, right, end)[0:1])

    def base_of(rot, level):
        off = 0
        for n in range(level):
            off = off + bits[(rot + n) % 3] * HALVES[n + 1]
        return off

    def axis_of(rot, level):
        return mate if level == 0 else flip[(rot + level - 1) % 3]

    def reduce_copy(t, j, level):
        size, cols = HALVES[level], pl.ds(j * WIDTH, WIDTH)
        if level == 0:
            source = part.at[9 + t % 2, :, cols]
            dev = mate
        else:
            rot = t + j
            off = base_of(rot, level - 1) + (1 - bits[(rot + level - 1) % 3]) * size
            source = part.at[t, pl.ds(pl.multiple_of(off, 32), size), cols]
            dev = axis_of(rot, level)
        sent = send_sem.at[t] if level else give_sem.at[t % 2]
        return pltpu.make_async_remote_copy(source, halves[level].at[t, :, cols], sent, recv_sem.at[t, j, level], device_id=dev, device_id_type=MESH)

    def gather_copy(w, t, j, level):
        rot = t + j
        off = core * 256 + base_of(rot, level)
        view = full[w].at[ORDER[t], pl.ds(pl.multiple_of(off, 32), HALVES[level]), pl.ds(j * WIDTH, WIDTH)]
        n = 7 - level
        return pltpu.make_async_remote_copy(view, view, send_sem.at[t], recv_sem.at[t, j, n], device_id=axis_of(rot, level), device_id_type=MESH)

    def wait_give(slot):
        view = part.at[9 + slot]
        pltpu.make_async_remote_copy(view, view, give_sem.at[slot], recv_sem.at[0, 0, 0], device_id=mate, device_id_type=MESH).wait_send()

    closing = set({key[:2]: key for slot in slots for key in slot if key[3] == 7}.values())

    def event(w, t, j, s):
        if s <= 3:
            reduce_copy(t, j, s).wait_recv()
            cols = slice(j * WIDTH, (j + 1) * WIDTH)
            off = base_of(t + j, s)
            rows = pl.ds(pl.multiple_of(off, 32), HALVES[s]) if s else slice(0, 256)
            total = part[t, rows, cols] + halves[s][t, :, cols]
            if s < 3:
                part[t, rows, cols] = total
                reduce_copy(t, j, s + 1).start()
            else:
                full[w][ORDER[t], pl.ds(pl.multiple_of(core * 256 + off, 32), HALVES[3]), cols] = total
                gather_copy(w, t, j, 3).start()
        else:
            gather_copy(w, t, j, 7 - s).wait_recv()
            if s < 7:
                gather_copy(w, t, j, 6 - s).start()
            elif (w, t, j, s) in closing:
                view = full[w].at[pl.ds(0, 2), pl.ds(0, 352)]
                pltpu.make_async_remote_copy(view, view, send_sem.at[t], recv_sem.at[t, j, 7], device_id=mate, device_id_type=MESH).wait_send()

    def pump(n, base, lo, hi):
        if not any(slots[base + m] for m in range(lo, hi)):
            return
        if hi - lo == 1:
            for key in slots[base + lo]:
                event(*key)
            return
        half = (lo + hi) // 2

        @pl.when(n < half)
        def _():
            pump(n, base, lo, half)

        @pl.when(n >= half)
        def _():
            pump(n, base, half, hi)

    def tap_half(n, place, row_at, plane):
        second = n % 2
        rows = pl.ds(pl.multiple_of(core * 256 + (1 - second) * (1 - 2 * core) * 256, 256), 256)

        @pl.when((second == 0) & (place >= 2))
        def _():
            wait_give(place % 2)

        grad = plane[pl.ds(row_at, ROWS)].reshape(PIX, CH)
        part[second * place + (1 - second) * (9 + place % 2)] = lax.dot_general(lv[:, rows], grad, (((0,), (0,)), ((), ())), preferred_element_type=F32)

        @pl.when(second == 0)
        def _():
            for j in range(PARTS):
                reduce_copy(place, j, 0).start()

    def last_sends():
        wait_give(1)
        wait_give(0)

    def tap_loops(u, base):
        def middle(n, _):
            if u == 0:
                @pl.when(n == 1)
                def _():
                    with mark("gelu"):
                        gelu_half(1, False)

                @pl.when(n == 0)
                def _():
                    with mark("gelu"):
                        gelu_half(0, True)
                    with mark("barrier"):
                        pl.semaphore_wait(barrier, 4 + near_count)
                        send_rows(0)
                        g_load.wait()
                        send_cols(0)
                        w_load.start()
                        stage_copy(0, 0).start()

            @pl.when(n == 2)
            def _():
                with mark("rows"):
                    wait_rows(u)

            row_at = (n // 2 + 1) % 3
            with mark("center"):
                tap_half(n, n // 2, row_at, centers[u])
            with mark("pump"):
                pump(n, base, 0, 6)
            return 0

        def side(n, _):
            @pl.when(n == 0)
            def _():
                with mark("cols"):
                    wait_cols(u)
                build_shift(u, 1)

            @pl.when(n == 6)
            def _():
                build_shift(u, 0)

            which = n // 6
            row_at = (n // 2 % 3 + 1) % 3
            with mark("side"):
                tap_half(n, 3 + n // 2, row_at, sh.at[1 - which])
            with mark("pump"):
                pump(n, base + 6, 0, 12)
            return 0

        lax.fori_loop(0, 6, middle, 0)
        lax.fori_loop(0, 12, side, 0)

    def conv_rows(g, center):
        lhs = []
        rhs = []
        for k in range(9):
            a, c = k // 3, k % 3
            plane = (sh.at[1], center, sh.at[0])[c]
            lhs.append(plane[pl.ds(g * GROUP + 2 - a, GROUP)].reshape(GPIX, CH))
            rhs.append(wbuf[k])
        return lax.dot_general(jnp.concatenate(lhs, axis=1), jnp.concatenate(rhs, axis=1), (((1,), (1,)), ((), ())), preferred_element_type=F32)

    def group_of(gi):
        return jnp.where(gi == 0, 0, jnp.where(gi == 1, NGROUP - 1, gi - 1))

    def stage_copy(gi, slot):
        return pltpu.make_async_copy(a_ref.at[pl.ds(group_of(gi) * GROUP, GROUP)], stage.at[slot], stage_sem.at[slot])

    def slope_rows(gi, slot):
        a_val = stage[slot].reshape(GPIX, CH).astype(F32)
        d_a = (dzs[...] * gelu_slope(a_val)).astype(BF16)
        dc[pl.ds(group_of(gi) * GROUP + 1, GROUP)] = d_a.reshape(GROUP, COLS, CH)

    def gelu_half(second, first):
        chans = pl.ds(pl.multiple_of(core * 256 + (1 - second) * (1 - 2 * core) * 256, 256), 256)

        def gelu_row(r, _):
            lv[pl.ds(pl.multiple_of(r * COLS, COLS), COLS), chans] = gelu_val(sh[0, r, :, chans].astype(F32)).astype(BF16)
            return 0

        for part_n in range(3):
            if first:
                a_loads[part_n].wait()
            lax.fori_loop(part_n * third, (part_n + 1) * third, gelu_row, 0)

    g_load.start()
    dzs[...] = jnp.zeros((GPIX, CH), F32)

    tap_loops(0, 0)

    x_load = pltpu.make_async_copy(x_ref, lv, load_sem.at[0])
    x_load.start()
    w_load.wait()

    stage_copy(0, 0).wait()

    def dz_step(gi, _):
        before = jnp.maximum(gi - 1, 0)
        slot = before % 2

        @pl.when(gi >= 2)
        def _():
            stage_copy(before, slot).wait()

        @pl.when(gi >= 1)
        def _():
            stage_copy(gi, gi % 2).start()

        with mark("dz"):
            slope_rows(before, slot)
            dzs[...] = conv_rows(group_of(gi), mid)

        @pl.when(gi == 2)
        def _():
            send_rows(1)

        with mark("pump"):
            pump(gi, 18, 0, NGROUP)
        return 0

    lax.fori_loop(0, NGROUP, dz_step, 0)
    w1_load = pltpu.make_async_copy(w1_ref, wbuf, load_sem.at[1])
    w1_load.start()
    last_sends()
    with mark("between"):
        stage_copy(NGROUP - 1, (NGROUP - 1) % 2).wait()
        slope_rows(NGROUP - 1, (NGROUP - 1) % 2)
        send_cols(1)
        x_load.wait()

    tap_loops(1, 18 + NGROUP)

    w1_load.wait()

    def dx_step(g, _):
        with mark("dx"):
            val = conv_rows(g, dc) + mid[pl.ds(g * GROUP + 1, GROUP)].reshape(GPIX, CH).astype(F32)
            lv[pl.ds(pl.multiple_of(g * GPIX, GPIX), GPIX)] = val.astype(BF16)
        with mark("pump"):
            pump(g, 36 + NGROUP, 0, NGROUP)
        return 0

    lax.fori_loop(0, NGROUP, dx_step, 0)
    last_sends()
    for key in slots[36 + 2 * NGROUP]:
        with mark("e%d%d%d%d" % key):
            event(*key)


def write_out(lv, full_one, full_two, dx_ref, dw1_ref, dw2_ref, sem):
    copies = [pltpu.make_async_copy(lv.at[pl.ds(k * 512, 512)], dx_ref.at[pl.ds(k * 512, 512)], sem.at[k]) for k in range(9)]
    copies += [pltpu.make_async_copy(full_one.at[k], dw1_ref.at[k], sem.at[9 + k]) for k in range(9)]
    copies += [pltpu.make_async_copy(full_two.at[k], dw2_ref.at[k], sem.at[18 + k]) for k in range(9)]
    for copy in copies:
        copy.start()
    for copy in copies:
        copy.wait()


def solution(mesh):
    slots, _ = build_slots((1, 0, 2, 3, 2, 3, 0, 2), (3, 3, 1, 1, 0, 2, 3, 3), slack=0.3)
    any_spec = pl.BlockSpec(memory_space=pl.ANY)
    vmem_spec = pl.BlockSpec(memory_space=pltpu.VMEM)

    def local_step(x_tile, a_tile, g_tile, w_one, w_two):
        lv, full_one, full_two = pl.pallas_call(
            functools.partial(kernel, slots),
            out_shape=(pltpu.VMEM((PIX, CH), BF16), pltpu.VMEM((9, CH, CH), F32), pltpu.VMEM((9, CH, CH), F32)),
            in_specs=[any_spec] * 5,
            out_specs=[vmem_spec] * 3,
            scratch_shapes=[
                pltpu.VMEM((11, 256, CH), F32),
                pltpu.VMEM((9, 256, CH), F32),
                pltpu.VMEM((9, 128, CH), F32),
                pltpu.VMEM((9, 64, CH), F32),
                pltpu.VMEM((9, 32, CH), F32),
                pltpu.VMEM((ROWS + 2, COLS, CH), BF16),
                pltpu.VMEM((ROWS + 2, COLS, CH), BF16),
                pltpu.VMEM((2, ROWS + 2, COLS, CH), BF16),
                pltpu.VMEM((9, CH, CH), BF16),
                pltpu.VMEM((2, GROUP, COLS, CH), BF16),
                pltpu.VMEM((2, 2, ROWS, CH), F32),
                pltpu.VMEM((2, 2, 8, CH), F32),
                pltpu.SemaphoreType.DMA((9,)),
                pltpu.SemaphoreType.DMA((2,)),
                pltpu.SemaphoreType.DMA((9, PARTS, 8)),
                pltpu.SemaphoreType.DMA((16,)),
                pltpu.SemaphoreType.DMA((16,)),
                pltpu.SemaphoreType.DMA((5,)),
                pltpu.SemaphoreType.DMA((2,)),
            ],
            compiler_params=pltpu.CompilerParams(collective_id=0, has_side_effects=True, vmem_limit_bytes=43440000),
        )(x_tile.reshape(PIX, CH), a_tile.reshape(ROWS, COLS, CH), g_tile.reshape(ROWS, COLS, CH), w_one.reshape(9, CH, CH), w_two.reshape(9, CH, CH))
        d_x, d_w1, d_w2 = pl.pallas_call(
            write_out,
            out_shape=(jax.ShapeDtypeStruct((PIX, CH), BF16), jax.ShapeDtypeStruct((9, CH, CH), F32), jax.ShapeDtypeStruct((9, CH, CH), F32)),
            in_specs=[vmem_spec] * 3,
            out_specs=[any_spec] * 3,
            scratch_shapes=[pltpu.SemaphoreType.DMA((27,))],
            compiler_params=pltpu.CompilerParams(vmem_limit_bytes=4000000),
        )(lv, full_one, full_two)
        return d_x.reshape(1, ROWS, COLS, CH), d_w1.reshape(3, 3, CH, CH), d_w2.reshape(3, 3, CH, CH)

    tile_spec = P(None, "row", "col", None)
    return jax.shard_map(local_step, mesh=mesh, in_specs=(tile_spec, tile_spec, tile_spec, P(), P()), out_specs=(tile_spec, P(), P()), check_vma=False)
```
